128 devices in a mesh: row: 8 (over z_hi, x), col: 16 (over z_lo, y, core).
Axes of the slice: x: 4, y: 4, z: 4 (z_hi: 2, z_lo: 2; z = z_hi * 2 + z_lo), core: 2. Of those that a mesh axis runs over, the one named last changes fastest.
Arguments:
- left_features: bfloat16 [768, 4096], P(('row', 'col')), may hold values from -6 to 6
- right_features: bfloat16 [768, 4096], P(('row', 'col')), may hold values from -6 to 6
- weight: bfloat16 [1024, 128], replicated, may hold values from -2 to 2
- bias: float32 [128], replicated, may hold values from -3 to 3
- upstream: bfloat16 [768, 768, 128], P('row', 'col'), may hold values from -0.59765625 to 0.59765625
Outputs:
- pair_out: bfloat16 [768, 768, 128], P('row', 'col')
- grad_left: bfloat16 [768, 4096], P(('row', 'col'))
- grad_right: bfloat16 [768, 4096], P(('row', 'col'))
- grad_weight: float32 [1024, 128], replicated
- grad_bias: float32 [128], replicated
The draws below stay inside these ranges and needn't reach their ends.
All inputs are finite; a program needn't handle non-finite values.
Results may differ from the reference program's by a relative error of at most 0.0063.
Values may be sent and summed in bfloat16 or wider, within the bound.
No kernel may reach another device: no remote copies, remote signals or barrier semaphores. Data moves between devices by JAX's collectives and lax.ppermute only.
A program may use at most 128 MiB of HBM per device.

```python
import jax
import jax.numpy as jnp
from jax import lax

CH = 32
PAIR = 128
SEQS = 128
RES = 768


def steps_of(key, shape, pieces, least, top_value):
    factor_of, own = 1.0, jax.random.fold_in(key, 6)
    for position, blocks in pieces:
        draws = jnp.exp(jax.random.uniform(jax.random.fold_in(own, position), (blocks,), jnp.float32, least / len(pieces), top_value / len(pieces)))
        factor_of = factor_of * jnp.repeat(draws, shape[position] // blocks).reshape([-1 if axis == position else 1 for axis in range(len(shape))])
    return factor_of


def scatter_about(rng, dims, spread, limit, shards=(), kind=jnp.bfloat16):
    array = spread * jax.random.normal(rng, dims, jnp.float32)
    if shards:
        array = array * steps_of(rng, dims, shards, -0.22, 0.18)
    return jnp.clip(array, -limit, limit).astype(kind)


def setup_inputs(seed: int = 0) -> dict:
    seeds = jax.random.split(jax.random.key(seed), 6)
    return {
        "left_features": scatter_about(seeds[0], (RES, SEQS * CH), 1.0, 6.0, ((0, 128),)),
        "right_features": scatter_about(seeds[1], (RES, SEQS * CH), 1.0, 6.0, ((0, 128),)),
        "weight": scatter_about(seeds[2], (CH * CH, PAIR), (CH * CH // SEQS) ** -0.5, 2.0),
        "bias": scatter_about(seeds[3], (PAIR,), 0.5, 3.0, (), jnp.float32),
        "upstream": scatter_about(seeds[4], (RES, RES, PAIR), 0.1, 0.59765625, ((0, 8), (1, 16))),
    }


block_rows = 16


def outer_product(rows, columns):
    rows3 = rows.astype(jnp.float32).reshape(rows.shape[0], SEQS, CH)
    cols3 = columns.astype(jnp.float32).reshape(columns.shape[0], SEQS, CH)
    product = jnp.einsum("isc,jsd->ijcd", rows3, cols3, precision=lax.Precision.HIGHEST) * (1.0 / SEQS)
    return product.reshape(rows.shape[0] * columns.shape[0], CH * CH).astype(jnp.bfloat16)


def reference(left_features, right_features, weight, bias, upstream):
    blocks = RES // block_rows

    def forward_block(index):
        rows = lax.dynamic_slice_in_dim(left_features, (index * block_rows).astype(jnp.int32), block_rows, 0)
        outer = outer_product(rows, right_features)
        return jnp.dot(outer, weight, preferred_element_type=jnp.float32) + bias

    pre = lax.map(forward_block, jnp.arange(blocks, dtype=jnp.int32)).reshape(RES, RES, PAIR)
    active = jnp.maximum(pre, 0.0)
    squared = active * active
    pair_out = ((squared + squared.transpose(1, 0, 2)) * 0.5).astype(jnp.bfloat16)
    grads = upstream.astype(jnp.float32)
    d_direct = (active * grads).astype(jnp.bfloat16)
    d_mirror = (active * grads.transpose(1, 0, 2)).astype(jnp.bfloat16)
    right3 = right_features.astype(jnp.float32).reshape(RES, SEQS, CH)
    weight_t = weight.T

    def backward_block(carry, index):
        d_right, d_weight, d_bias = carry
        start = (index * block_rows).astype(jnp.int32)
        rows = lax.dynamic_slice_in_dim(left_features, start, block_rows, 0)
        rows3 = rows.astype(jnp.float32).reshape(block_rows, SEQS, CH)
        outer = outer_product(rows, right_features)
        part_direct = lax.dynamic_slice_in_dim(d_direct, start, block_rows, 0).reshape(-1, PAIR)
        part_mirror = lax.dynamic_slice_in_dim(d_mirror, start, block_rows, 0).reshape(-1, PAIR)
        g_direct = jnp.dot(part_direct, weight_t, preferred_element_type=jnp.float32).astype(jnp.bfloat16)
        g_mirror = jnp.dot(part_mirror, weight_t, preferred_element_type=jnp.float32).astype(jnp.bfloat16)
        total = (g_direct.astype(jnp.float32) + g_mirror.astype(jnp.float32)).reshape(block_rows, RES, CH, CH)
        d_left = jnp.einsum("ijcd,jsd->isc", total, right3, precision=lax.Precision.HIGHEST) * (1.0 / SEQS)
        d_right = d_right + jnp.einsum("ijcd,isc->jsd", total, rows3, precision=lax.Precision.HIGHEST) * (1.0 / SEQS)
        d_weight = d_weight + jnp.dot(outer.T, part_direct, preferred_element_type=jnp.float32)
        d_weight = d_weight + jnp.dot(outer.T, part_mirror, preferred_element_type=jnp.float32)
        d_bias = d_bias + jnp.sum(part_direct.astype(jnp.float32), axis=0) + jnp.sum(part_mirror.astype(jnp.float32), axis=0)
        return (d_right, d_weight, d_bias), d_left.reshape(block_rows, SEQS * CH)

    init = (jnp.zeros((RES, SEQS, CH), jnp.float32), jnp.zeros((CH * CH, PAIR), jnp.float32), jnp.zeros((PAIR,), jnp.float32))
    (d_right, d_weight, d_bias), d_left = lax.scan(backward_block, init, jnp.arange(blocks, dtype=jnp.int32))
    grad_left = d_left.reshape(RES, SEQS * CH).astype(jnp.bfloat16)
    grad_right = d_right.reshape(RES, SEQS * CH).astype(jnp.bfloat16)
    return pair_out, grad_left, grad_right, d_weight, d_bias
```

```python
import functools

import jax
import jax.numpy as jnp
from jax import lax
from jax.experimental import pallas as pl
from jax.experimental.pallas import tpu as pltpu
from jax.sharding import PartitionSpec as P

CH = 32
SEQS = 128
GROUP = 4
BLOCK = 32
BF16 = jnp.bfloat16
F32 = jnp.float32


def contract(a, b, dims):
    numbers = (((dims[0],), (dims[1],)), ((), ()))
    return lax.dot_general(a, b, numbers, preferred_element_type=F32)


def spread(parts, places, turn):
    p0, p1, p2, p3 = (parts[(p - turn) % GROUP] for p in range(GROUP))
    odd, high = places
    return jnp.where(high, jnp.where(odd, p3, p2), jnp.where(odd, p1, p0))


def pair_kernel(
    steps,
    across,
    lane_ref,
    row_ref,
    weight_ref,
    bias_ref,
    up_ref,
    pair_ref,
    dlane_ref,
    drow_ref,
    dweight_ref,
    dbias_ref,
    squares,
    products,
    packed,
    grads,
    row_t,
    drow_acc,
    dweight_acc,
    dbias_acc,
):
    term, step = pl.program_id(0), pl.program_id(1)
    quarters = CH // GROUP
    groups = BLOCK // GROUP
    depth = quarters * across
    scale = 1.0 / SEQS
    lane = lax.broadcasted_iota(jnp.int32, (across, 128), 1) // CH
    places = (lane % 2 == 1, lane >= 2)

    @pl.when(step == 0)
    def _():
        for m in range(GROUP):
            row_t[m] = row_ref[0, m * depth : (m + 1) * depth, :].T
        drow_acc[...] = jnp.zeros_like(drow_acc)
        dweight_acc[...] = jnp.zeros_like(dweight_acc)

    @pl.when((step == 0) & (term == 0))
    def _():
        dbias_acc[...] = jnp.zeros_like(dbias_acc)

    def turned_lanes(m):
        return jnp.concatenate(
            [
                lane_ref[0, pl.ds((GROUP * g + (p - m) % GROUP) * CH, CH), :]
                for g in range(groups)
                for p in range(GROUP)
            ],
            axis=0,
        )

    def turned_weight(q):
        return jnp.concatenate(
            [
                weight_ref[0, pl.ds((GROUP * k + (p - q) % GROUP) * CH, CH), :]
                for k in range(quarters)
                for p in range(GROUP)
            ],
            axis=0,
        )

    for m in range(GROUP):
        outer = contract(row_ref[0, m * depth : (m + 1) * depth, :], turned_lanes(m), (1, 1))
        products[m] = (outer * scale).astype(BF16)
    for k in range(quarters):
        for g in range(groups):
            rows, lanes = pl.ds(k * across, across), pl.ds(g * 128, 128)
            parts = [products[m, rows, lanes] for m in range(GROUP)]
            for q in range(GROUP):
                packed[q, pl.ds(g * across, across), pl.ds(k * 128, 128)] = spread(parts, places, q)
    for q in range(GROUP):
        outer = packed[q]
        weight_q = turned_weight(q)
        pre = jnp.dot(outer, weight_q, preferred_element_type=F32) + bias_ref[...]
        active = jnp.maximum(pre, 0.0)
        squared = active * active
        up = jnp.concatenate([up_ref[GROUP * g + q] for g in range(groups)], axis=0)
        d_pre = (active * up.astype(F32)).astype(BF16)

        @pl.when(term == 0)
        def _():
            for g in range(groups):
                squares[step * BLOCK + GROUP * g + q] = squared[g * across : (g + 1) * across]

        @pl.when(term == 1)
        def _():
            for g in range(groups):
                both = squared[g * across : (g + 1) * across] + squares[step * BLOCK + GROUP * g + q]
                pair_ref[GROUP * g + q] = (both * 0.5).astype(BF16)

        products[q] = contract(d_pre, weight_q, (1, 1)).astype(BF16)
        dweight_acc[q] += contract(d_pre, outer, (0, 0))
        dbias_acc[...] += jnp.sum(
            d_pre.astype(F32).reshape(groups * across // 8, 8, 128), axis=0
        )
    for k in range(quarters):
        for g in range(groups):
            parts = [
                products[q, pl.ds(g * across, across), pl.ds(k * 128, 128)] for q in range(GROUP)
            ]
            rows, lanes = pl.ds(k * across, across), pl.ds(g * 128, 128)
            for m in range(GROUP):
                grads[m, rows, lanes] = spread(parts, places, m)

    def unturned(wide, turn):
        if turn == 0:
            return wide
        return jnp.concatenate(
            [
                pltpu.roll(wide[:, n * 128 : (n + 1) * 128], 128 - CH * turn, 1)
                for n in range(wide.shape[1] // 128)
            ],
            axis=1,
        )

    d_lane = None
    for m in range(GROUP):
        drow_acc[m * depth : (m + 1) * depth, :] += jnp.dot(
            grads[m], turned_lanes(m), preferred_element_type=F32
        )
        one = unturned(jnp.dot(row_t[m], grads[m], preferred_element_type=F32), m)
        d_lane = one if d_lane is None else d_lane + one
    dlane_ref[0] = (d_lane.T * scale).astype(BF16)

    @pl.when(step == steps - 1)
    def _():
        drow_ref[0] = (drow_acc[...] * scale).astype(BF16)
        total = dweight_acc[0]
        for q in range(1, GROUP):
            total = total + unturned(dweight_acc[q], q)
        flat = total.T

        @pl.when(term == 0)
        def _():
            for k in range(CH):
                dweight_ref[pl.ds(k, CH, stride=CH), :] = flat[k * CH : (k + 1) * CH]

        @pl.when(term == 1)
        def _():
            dweight_ref[...] += flat
            dbias_ref[...] = dbias_acc[...]


def pair_block(lanes, rows, weights, bias, upstream):
    count, across, pairs = upstream.shape
    steps = count // BLOCK
    width = BLOCK * CH
    depth = CH // GROUP * across
    once = lambda t, s: (0, 0)
    return pl.pallas_call(
        functools.partial(pair_kernel, steps, across),
        grid=(2, steps),
        in_specs=[
            pl.BlockSpec((1, width, SEQS), lambda t, s: (t, s, 0)),
            pl.BlockSpec((1, CH * across, SEQS), lambda t, s: (t, 0, 0)),
            pl.BlockSpec((1, CH * CH, pairs), lambda t, s: (t, 0, 0)),
            pl.BlockSpec((1, pairs), once),
            pl.BlockSpec((BLOCK, across, pairs), lambda t, s: (s, 0, 0)),
        ],
        out_specs=[
            pl.BlockSpec((BLOCK, across, pairs), lambda t, s: (t * s, 0, 0)),
            pl.BlockSpec((1, width, SEQS), lambda t, s: (t, s, 0)),
            pl.BlockSpec((1, CH * across, SEQS), lambda t, s: (t, 0, 0)),
            pl.BlockSpec((CH * CH, pairs), once),
            pl.BlockSpec((8, pairs), once),
        ],
        out_shape=[
            jax.ShapeDtypeStruct((count, across, pairs), BF16),
            jax.ShapeDtypeStruct((2, count * CH, SEQS), BF16),
            jax.ShapeDtypeStruct((2, CH * across, SEQS), BF16),
            jax.ShapeDtypeStruct((CH * CH, pairs), F32),
            jax.ShapeDtypeStruct((8, pairs), F32),
        ],
        scratch_shapes=[
            pltpu.VMEM((count, across, pairs), F32),
            pltpu.VMEM((GROUP, depth, width), BF16),
            pltpu.VMEM((GROUP, BLOCK // GROUP * across, CH * CH), BF16),
            pltpu.VMEM((GROUP, depth, width), BF16),
            pltpu.VMEM((GROUP, SEQS, depth), BF16),
            pltpu.VMEM((CH * across, SEQS), F32),
            pltpu.VMEM((GROUP, pairs, CH * CH), F32),
            pltpu.VMEM((8, pairs), F32),
        ],
        compiler_params=pltpu.CompilerParams(vmem_limit_bytes=60 * 1024 * 1024),
        cost_estimate=pl.CostEstimate(
            flops=12 * count * across * CH * CH * SEQS * 2,
            bytes_accessed=16 * 1024 * 1024,
            transcendentals=0,
        ),
    )(lanes, rows, weights, bias, upstream)


def exchange(x, axis):
    return lax.all_to_all(x, axis, split_axis=0, concat_axis=0, tiled=True)


def everywhere(x, axis):
    members = lax.axis_size(axis)
    return exchange(jnp.broadcast_to(x[None], (members,) + x.shape), axis)


def local(left_features, right_features, weight, bias, upstream):
    rows_n, cols_n = lax.axis_size("row"), lax.axis_size("col")
    own, pairs = left_features.shape[0], weight.shape[1]
    count, across = upstream.shape[0], upstream.shape[1]
    to_part = [(o, (o % rows_n) * cols_n + o // rows_n) for o in range(rows_n * cols_n)]
    to_owner = [(b, a) for a, b in to_part]
    both = ("row", "col")

    def channels_first(x):
        return x.reshape(own, SEQS, CH).transpose(0, 2, 1)

    mine = jnp.stack([channels_first(left_features), channels_first(right_features)])
    mine = mine.reshape(2, own * CH, SEQS)
    part = lax.ppermute(mine, both, to_part)
    lanes = everywhere(mine, "col").transpose(1, 0, 2, 3).reshape(2, count * CH, SEQS)
    rows = everywhere(part, "row").reshape(rows_n, 2, own, CH // GROUP, GROUP, SEQS)
    rows = rows[:, ::-1].transpose(1, 4, 3, 0, 2, 5).reshape(2, CH * across, SEQS)
    weights = jnp.stack(
        [weight.reshape(CH, CH, pairs).transpose(1, 0, 2).reshape(CH * CH, pairs), weight]
    )
    pair_out, d_lanes, d_rows, d_weight, d_bias = pair_block(
        lanes, rows, weights, bias.reshape(1, pairs), upstream
    )
    d_rows = d_rows.reshape(2, GROUP, CH // GROUP, rows_n, own, SEQS)[::-1]
    d_rows = d_rows.transpose(3, 0, 4, 2, 1, 5).reshape(rows_n, 2 * own * CH, SEQS)
    d_bias = jnp.sum(d_bias, axis=0, keepdims=True)

    def two_parts(x):
        high = x.astype(BF16)
        low = (x - high.astype(F32)).astype(BF16)
        return jnp.concatenate([high, low, jnp.zeros((14, pairs), BF16)], axis=0)

    def one_part(x):
        return jnp.sum(x[:2], axis=0, keepdims=True)

    slices = d_weight.reshape(rows_n, CH * CH // rows_n, pairs).astype(BF16)
    bias_rows = jnp.broadcast_to(two_parts(d_bias)[None], (rows_n, 16, pairs))
    sent = exchange(jnp.concatenate([d_rows, slices, bias_rows], axis=1), "row")
    summed = jnp.sum(sent.astype(F32), axis=0)
    n_own = 2 * own * CH
    n_slice = CH * CH // rows_n
    part_grads = lax.ppermute(summed[:n_own].astype(BF16), both, to_owner)
    slice_sum = summed[n_own : n_own + n_slice].astype(BF16)
    bias_sum = two_parts(one_part(summed[n_own + n_slice :]))
    d_lanes = d_lanes.reshape(2, cols_n, own * CH, SEQS).transpose(1, 0, 2, 3)
    d_lanes = d_lanes.reshape(cols_n, n_own, SEQS)
    shared = jnp.concatenate([slice_sum, bias_sum], axis=0)
    shared = jnp.broadcast_to(shared[None], (cols_n,) + shared.shape)
    sent = exchange(jnp.concatenate([d_lanes, shared], axis=1), "col")
    summed = jnp.sum(sent.astype(F32), axis=0)
    grads = summed[:n_own] + part_grads.astype(F32)
    grad_slice = summed[n_own : n_own + n_slice]
    grad_bias = one_part(summed[n_own + n_slice :]).reshape(pairs)
    grad_weight = everywhere(grad_slice, "row").reshape(CH * CH, pairs)
    grads = grads.reshape(2, own, CH, SEQS).transpose(0, 1, 3, 2).reshape(2, own, SEQS * CH)
    grads = grads.astype(BF16)
    return pair_out, grads[0], grads[1], grad_weight, grad_bias


def solution(mesh):
    placed = (P(("row", "col"), None), P(("row", "col"), None), P(), P(), P("row", "col", None))
    return jax.shard_map(
        local,
        mesh=mesh,
        in_specs=placed,
        out_specs=(
            P("row", "col", None),
            P(("row", "col"), None),
            P(("row", "col"), None),
            P(),
            P(),
        ),
        check_vma=False,
    )
```

```python
import functools

import jax
import jax.numpy as jnp
from jax import lax
from jax.experimental import pallas as pl
from jax.experimental.pallas import tpu as pltpu
from jax.sharding import PartitionSpec as P


CH = 32
SEQS = 128
GROUP = 4
BLOCK = 32
TILE = 16
BF16 = jnp.bfloat16
F32 = jnp.float32


def contract(a, b, dims):
    numbers = (((dims[0],), (dims[1],)), ((), ()))
    return lax.dot_general(a, b, numbers, preferred_element_type=F32)


def spread(parts, odd, high):
    once = [jnp.where(odd, parts[(r + 1) % GROUP], parts[r]) for r in range(GROUP)]
    twice = [jnp.where(high, once[(r + 2) % GROUP], once[r]) for r in range(GROUP)]
    return [twice[-q % GROUP] for q in range(GROUP)]


def to_tiles(ref, at, wide):
    for n in range(wide.shape[1] // 128):
        ref[at, n] = wide[:, n * 128 : (n + 1) * 128]


def from_tiles(ref, at, first=0, count=None):
    count = ref.shape[1] if count is None else count
    return jnp.concatenate([ref[at, first + n] for n in range(count)], axis=1)


def pair_kernel(
    steps,
    across,
    lane_ref,
    row_ref,
    weight_ref,
    bias_ref,
    up_ref,
    pair_ref,
    cols_ref,
    send_ref,
    squares,
    products,
    packed,
    grads,
    row_t,
    drow_acc,
    dweight_acc,
    dweight_sum,
    drow_turned,
    dbias_acc,
):
    term, step = pl.program_id(0), pl.program_id(1)
    quarters = CH // GROUP
    groups = BLOCK // GROUP
    depth = quarters * across
    scale = 1.0 / SEQS
    own = across // send_ref.shape[0]
    lane = lax.broadcasted_iota(jnp.int32, (TILE, 128), 1) // CH
    odd = (lane % 2).astype(F32).astype(BF16) > 0.5
    high = (lane // 2).astype(F32).astype(BF16) > 0.5

    @pl.when(step == 0)
    def _():
        for m in range(GROUP):
            row_t[m] = row_ref[0, m * depth : (m + 1) * depth, :].T
        drow_acc[...] = jnp.zeros_like(drow_acc)
        dweight_acc[...] = jnp.zeros_like(dweight_acc)

    @pl.when((step == 0) & (term == 0))
    def _():
        dbias_acc[...] = jnp.zeros_like(dbias_acc)

    def turned_lanes(m):
        return jnp.concatenate(
            [
                lane_ref[0, pl.ds((GROUP * g + (p - m) % GROUP) * CH, CH), :]
                for g in range(groups)
                for p in range(GROUP)
            ],
            axis=0,
        )

    def turned_weight(q):
        return jnp.concatenate(
            [
                weight_ref[0, pl.ds((GROUP * k + (p - q) % GROUP) * CH, CH), :]
                for k in range(quarters)
                for p in range(GROUP)
            ],
            axis=0,
        )

    for m in range(GROUP):
        outer = contract(row_ref[0, m * depth : (m + 1) * depth, :], turned_lanes(m), (1, 1))
        to_tiles(products, m, (outer * scale).astype(BF16))

    def by_pair(k, _):
        from_rows = pl.multiple_of(k * across, TILE)
        for g in range(groups):
            for t in range(0, across, TILE):
                parts = [
                    products[m, g, pl.ds(from_rows + t, TILE), :] for m in range(GROUP)
                ]
                for q, tile in enumerate(spread(parts, odd, high)):
                    packed[q, k, pl.ds(g * across + t, TILE), :] = tile
        return _

    lax.fori_loop(0, quarters, by_pair, 0)
    for q in range(GROUP):
        outer = from_tiles(packed, q)
        weight_q = turned_weight(q)
        pre = jnp.dot(outer, weight_q, preferred_element_type=F32) + bias_ref[...]
        active = jnp.maximum(pre, 0.0)
        squared = active * active
        up = jnp.concatenate([up_ref[GROUP * g + q] for g in range(groups)], axis=0)
        d_pre = (active * up.astype(F32)).astype(BF16)

        for g in range(groups):
            place = step * BLOCK + GROUP * g + q
            here = squared[g * across : (g + 1) * across]
            pair_ref[GROUP * g + q] = ((here + squares[place]) * 0.5).astype(BF16)
            squares[place] = here
        to_tiles(products, q, contract(d_pre, weight_q, (1, 1)).astype(BF16))
        dweight_acc[q] += contract(d_pre, outer, (0, 0))
        dbias_acc[...] += jnp.sum(
            d_pre.astype(F32).reshape(groups * across // 8, 8, 128), axis=0
        )

    def by_channel(k, _):
        to_rows = pl.multiple_of(k * across, TILE)
        for g in range(groups):
            for t in range(0, across, TILE):
                parts = [
                    products[q, k, pl.ds(g * across + t, TILE), :] for q in range(GROUP)
                ]
                for m, tile in enumerate(spread(parts, odd, high)):
                    grads[m, g, pl.ds(to_rows + t, TILE), :] = tile
        return _

    lax.fori_loop(0, quarters, by_channel, 0)

    def unturned(wide, turn):
        if turn == 0:
            return wide
        return jnp.concatenate(
            [
                pltpu.roll(wide[:, n * 128 : (n + 1) * 128], 128 - CH * turn, 1)
                for n in range(wide.shape[1] // 128)
            ],
            axis=1,
        )

    for n in range(0, BLOCK * CH, 256):
        d_lane = None
        for m in range(GROUP):
            wide = jnp.dot(
                row_t[m], from_tiles(grads, m, n // 128, 2), preferred_element_type=F32
            )
            wide = unturned(wide, m)
            d_lane = wide if d_lane is None else d_lane + wide
        d_lane = (d_lane.T * scale).astype(BF16)
        for r in range(256 // CH):
            residue = step * BLOCK + n // CH + r
            to_row = pl.multiple_of((term * own + residue % own) * CH, CH)
            cols_ref[residue // own, pl.ds(to_row, CH), :] = d_lane[r * CH : (r + 1) * CH]
    for m in range(GROUP):
        drow_acc[m * depth : (m + 1) * depth, :] += jnp.dot(
            from_tiles(grads, m), turned_lanes(m), preferred_element_type=F32
        )

    @pl.when(step == steps - 1)
    def _():
        for m in range(GROUP):
            for k in range(quarters):
                block = drow_acc[pl.ds(m * depth + k * across, across), :]
                drow_turned[pl.ds(k * GROUP + m, across, stride=CH), :] = block * scale
        sent = drow_turned[...].astype(BF16).reshape(send_ref.shape[0], -1, SEQS)
        count = sent.shape[1]
        total = dweight_acc[0]
        for q in range(1, GROUP):
            total = total + unturned(dweight_acc[q], q)
        flat = total.T

        @pl.when(term == 0)
        def _():
            send_ref[:, count : 2 * count, :] = sent
            for k in range(CH):
                dweight_sum[pl.ds(k, CH, stride=CH), :] = flat[k * CH : (k + 1) * CH]

        @pl.when(term == 1)
        def _():
            send_ref[:, :count, :] = sent
            whole = (dweight_sum[...] + flat).astype(BF16)
            peers = cols_ref.shape[0]
            end = 2 * count + whole.shape[0] // peers
            cols_ref[:, 2 * count : end, :] = whole.reshape(peers, -1, whole.shape[1])
            d_bias = jnp.sum(dbias_acc[...], axis=0, keepdims=True)
            first = d_bias.astype(BF16).astype(F32)
            place = lax.broadcasted_iota(jnp.int32, (TILE, 128), 0)
            rows = jnp.where(place == 0, first, jnp.where(place == 1, d_bias - first, 0.0))
            for r in range(peers):
                cols_ref[r, end : end + TILE, :] = rows.astype(BF16)


def pair_block(lanes, rows, weights, bias, upstream, row_peers, col_peers):
    count, across, pairs = upstream.shape
    steps = count // BLOCK
    width = BLOCK * CH
    depth = CH // GROUP * across
    once = lambda t, s: (0, 0)
    sent = 2 * CH * across // row_peers + CH * CH // col_peers + TILE
    return pl.pallas_call(
        functools.partial(pair_kernel, steps, across),
        grid=(2, steps),
        in_specs=[
            pl.BlockSpec((1, width, SEQS), lambda t, s: (t, s, 0)),
            pl.BlockSpec((1, CH * across, SEQS), lambda t, s: (t, 0, 0)),
            pl.BlockSpec((1, CH * CH, pairs), lambda t, s: (t, 0, 0)),
            pl.BlockSpec((1, pairs), once),
            pl.BlockSpec((BLOCK, across, pairs), lambda t, s: (s, 0, 0)),
        ],
        out_specs=[
            pl.BlockSpec((BLOCK, across, pairs), lambda t, s: (t * s, 0, 0)),
            pl.BlockSpec((col_peers, sent, SEQS), lambda t, s: (0, 0, 0)),
            pl.BlockSpec((row_peers, sent, SEQS), lambda t, s: (0, 0, 0)),
        ],
        out_shape=[
            jax.ShapeDtypeStruct((count, across, pairs), BF16),
            jax.ShapeDtypeStruct((col_peers, sent, SEQS), BF16),
            jax.ShapeDtypeStruct((row_peers, sent, SEQS), BF16),
        ],
        scratch_shapes=[
            pltpu.VMEM((count, across, pairs), F32),
            pltpu.VMEM((GROUP, width // 128, depth, 128), BF16),
            pltpu.VMEM((GROUP, width // 128, depth, 128), BF16),
            pltpu.VMEM((GROUP, width // 128, depth, 128), BF16),
            pltpu.VMEM((GROUP, SEQS, depth), BF16),
            pltpu.VMEM((CH * across, SEQS), F32),
            pltpu.VMEM((GROUP, pairs, CH * CH), F32),
            pltpu.VMEM((CH * CH, pairs), F32),
            pltpu.VMEM((CH * across, SEQS), F32),
            pltpu.VMEM((8, pairs), F32),
        ],
        compiler_params=pltpu.CompilerParams(vmem_limit_bytes=60 * 1024 * 1024),
        cost_estimate=pl.CostEstimate(
            flops=12 * count * across * CH * CH * SEQS * 2,
            bytes_accessed=16 * 1024 * 1024,
            transcendentals=0,
        ),
    )(lanes, rows, weights, bias, upstream)


def exchange(x, axis, groups=None):
    return lax.all_to_all(
        x, axis, split_axis=0, concat_axis=0, axis_index_groups=groups, tiled=True
    )


def everywhere(x, axis, groups=None):
    members = lax.axis_size(axis) if groups is None else len(groups[0])
    copies = jnp.broadcast_to(x[None], (members,) + x.shape)
    return exchange(copies, axis, groups)


def two_parts(x):
    high = x.astype(BF16)
    low = (x - high.astype(F32)).astype(BF16)
    return jnp.concatenate([high, low, jnp.zeros((TILE - 2, x.shape[1]), BF16)], axis=0)


def one_part(x):
    return jnp.sum(x[:2], axis=0, keepdims=True)


def local(left_features, right_features, weight, bias, upstream):
    rows_n, cols_n = lax.axis_size("row"), lax.axis_size("col")
    own, pairs = left_features.shape[0], weight.shape[1]
    count, across = upstream.shape[0], upstream.shape[1]
    to_part = [(o, (o % rows_n) * cols_n + o // rows_n) for o in range(rows_n * cols_n)]
    to_owner = [(b, a) for a, b in to_part]
    both = ("row", "col")
    same_core = [list(range(k, cols_n, 2)) for k in range(2)]
    other_core = [(k, k ^ 1) for k in range(cols_n)]
    n_own = 2 * own * CH

    def channels_first(x):
        return x.reshape(own, SEQS, CH).transpose(0, 2, 1)

    mine = jnp.stack([channels_first(left_features), channels_first(right_features)])
    mine = mine.reshape(2, own * CH, SEQS)
    part = lax.ppermute(mine, both, to_part)
    half = everywhere(mine, "col", same_core)
    other = lax.ppermute(half, "col", other_core)
    rows = everywhere(part, "row")
    second = lax.axis_index("col") % 2 == 1
    lanes = jnp.stack(
        [jnp.where(second, other, half), jnp.where(second, half, other)], axis=1
    )
    lanes = lanes.transpose(2, 0, 1, 3, 4).reshape(2, count * CH, SEQS)
    rows = rows.reshape(rows_n, 2, own, CH // GROUP, GROUP, SEQS)
    rows = rows[:, ::-1].transpose(1, 4, 3, 0, 2, 5).reshape(2, CH * across, SEQS)
    weights = jnp.stack(
        [weight.reshape(CH, CH, pairs).transpose(1, 0, 2).reshape(CH * CH, pairs), weight]
    )
    pair_out, to_cols, to_rows = pair_block(
        lanes, rows, weights, bias.reshape(1, pairs), upstream, rows_n, cols_n
    )
    n_slice = CH * CH // cols_n
    summed = jnp.sum(exchange(to_cols, "col").astype(F32), axis=0)
    grads = summed[:n_own]
    shared = jnp.concatenate(
        [summed[n_own : n_own + n_slice].astype(BF16), two_parts(one_part(summed[n_own + n_slice :]))],
        axis=0,
    )
    shared = jnp.broadcast_to(shared[None], (rows_n,) + shared.shape)
    to_rows = lax.dynamic_update_slice(to_rows, shared, (0, n_own, 0))
    summed = jnp.sum(exchange(to_rows, "row").astype(F32), axis=0)
    part_grads = lax.ppermute(summed[:n_own].astype(BF16), both, to_owner)
    grad_weight = everywhere(summed[n_own : n_own + n_slice], "col")
    grad_weight = grad_weight.reshape(CH * CH, pairs)
    grad_bias = one_part(summed[n_own + n_slice :]).reshape(pairs)
    grads = grads + part_grads.astype(F32)
    grads = grads.reshape(2, own, CH, SEQS).transpose(0, 1, 3, 2).reshape(2, own, SEQS * CH)
    grads = grads.astype(BF16)
    return pair_out, grads[0], grads[1], grad_weight, grad_bias


def solution(mesh):
    placed = (P(("row", "col"), None), P(("row", "col"), None), P(), P(), P("row", "col", None))
    return jax.shard_map(
        local,
        mesh=mesh,
        in_specs=placed,
        out_specs=(
            P("row", "col", None),
            P(("row", "col"), None),
            P(("row", "col"), None),
            P(),
            P(),
        ),
        check_vma=False,
    )
```

```python
import functools

import jax
import jax.numpy as jnp
from jax import lax
from jax.experimental import pallas as pl
from jax.experimental.pallas import tpu as pltpu
from jax.sharding import PartitionSpec as P


CH = 32
SEQS = 128
GROUP = 4
BLOCK = 32
TILE = 16
BF16 = jnp.bfloat16
F32 = jnp.float32


def contract(a, b, dims):
    numbers = (((dims[0],), (dims[1],)), ((), ()))
    return lax.dot_general(a, b, numbers, preferred_element_type=F32)


def spread(parts, odd, high):
    once = [jnp.where(odd, parts[(r + 1) % GROUP], parts[r]) for r in range(GROUP)]
    twice = [jnp.where(high, once[(r + 2) % GROUP], once[r]) for r in range(GROUP)]
    return [twice[-q % GROUP] for q in range(GROUP)]


def unturned(wide, turn):
    if turn == 0:
        return wide
    return jnp.concatenate(
        [
            pltpu.roll(wide[:, n * 128 : (n + 1) * 128], 128 - CH * turn, 1)
            for n in range(wide.shape[1] // 128)
        ],
        axis=1,
    )


def to_tiles(ref, at, wide):
    for n in range(wide.shape[1] // 128):
        ref[at, n] = wide[:, n * 128 : (n + 1) * 128]


def from_tiles(ref, at, first=0, count=None):
    count = ref.shape[1] if count is None else count
    return jnp.concatenate([ref[at, first + n] for n in range(count)], axis=1)


def pair_kernel(
    steps,
    across,
    lane_ref,
    row_ref,
    weight_ref,
    bias_ref,
    up_ref,
    pair_ref,
    grads_ref,
    send_ref,
    squares,
    products,
    packed,
    drow_acc,
    dweight_acc,
    dweight_sum,
    drow_turned,
    dbias_acc,
):
    term, step = pl.program_id(0), pl.program_id(1)
    quarters = CH // GROUP
    groups = BLOCK // GROUP
    depth = quarters * across
    scale = 1.0 / SEQS
    grads = grads_ref.at[0, 0]
    lane = lax.broadcasted_iota(jnp.int32, (TILE, 128), 1) // CH
    odd = (lane % 2).astype(F32).astype(BF16) > 0.5
    high = (lane // 2).astype(F32).astype(BF16) > 0.5

    @pl.when(step == 0)
    def _():
        drow_acc[...] = jnp.zeros_like(drow_acc)
        dweight_acc[...] = jnp.zeros_like(dweight_acc)

    @pl.when((step == 0) & (term == 0))
    def _():
        dbias_acc[...] = jnp.zeros_like(dbias_acc)

    def turned_lanes(m):
        return jnp.concatenate(
            [
                lane_ref[0, pl.ds((GROUP * g + (p - m) % GROUP) * CH, CH), :]
                for g in range(groups)
                for p in range(GROUP)
            ],
            axis=0,
        )

    def turned_weight(q):
        return jnp.concatenate(
            [
                weight_ref[0, pl.ds((GROUP * k + (p - q) % GROUP) * CH, CH), :]
                for k in range(quarters)
                for p in range(GROUP)
            ],
            axis=0,
        )

    for m in range(GROUP):
        outer = contract(row_ref[0, m * depth : (m + 1) * depth, :], turned_lanes(m), (1, 1))
        to_tiles(products, m, (outer * scale).astype(BF16))

    def by_pair(k, _):
        from_rows = pl.multiple_of(k * across, TILE)
        for g in range(groups):
            for t in range(0, across, TILE):
                parts = [
                    products[m, g, pl.ds(from_rows + t, TILE), :] for m in range(GROUP)
                ]
                for q, tile in enumerate(spread(parts, odd, high)):
                    packed[q, k, pl.ds(g * across + t, TILE), :] = tile
        return _

    lax.fori_loop(0, quarters, by_pair, 0)
    for q in range(GROUP):
        outer = from_tiles(packed, q)
        weight_q = turned_weight(q)
        pre = jnp.dot(outer, weight_q, preferred_element_type=F32) + bias_ref[...]
        active = jnp.maximum(pre, 0.0)
        squared = active * active
        up = jnp.concatenate([up_ref[GROUP * g + q] for g in range(groups)], axis=0)
        d_pre = (active * up.astype(F32)).astype(BF16)

        for g in range(groups):
            place = step * BLOCK + GROUP * g + q
            here = squared[g * across : (g + 1) * across]
            pair_ref[GROUP * g + q] = ((here + squares[place]) * 0.5).astype(BF16)
            squares[place] = here
        to_tiles(products, q, contract(d_pre, weight_q, (1, 1)).astype(BF16))
        dweight_acc[q] += contract(d_pre, outer, (0, 0))
        dbias_acc[...] += jnp.sum(
            d_pre.astype(F32).reshape(groups * across // 8, 8, 128), axis=0
        )

    def by_channel(k, _):
        to_rows = pl.multiple_of(k * across, TILE)
        for g in range(groups):
            for t in range(0, across, TILE):
                parts = [
                    products[q, k, pl.ds(g * across + t, TILE), :] for q in range(GROUP)
                ]
                for m, tile in enumerate(spread(parts, odd, high)):
                    grads[m, g, pl.ds(to_rows + t, TILE), :] = tile
        return _

    lax.fori_loop(0, quarters, by_channel, 0)

    for m in range(GROUP):
        drow_acc[m * depth : (m + 1) * depth, :] += jnp.dot(
            from_tiles(grads, m), turned_lanes(m), preferred_element_type=F32
        )

    @pl.when(step == steps - 1)
    def _():
        for m in range(GROUP):
            for k in range(quarters):
                block = drow_acc[pl.ds(m * depth + k * across, across), :]
                drow_turned[pl.ds(k * GROUP + m, across, stride=CH), :] = block * scale
        sent = drow_turned[...].astype(BF16).reshape(send_ref.shape[0], -1, SEQS)
        count = sent.shape[1]
        total = dweight_acc[0]
        for q in range(1, GROUP):
            total = total + unturned(dweight_acc[q], q)
        flat = total.T

        @pl.when(term == 0)
        def _():
            send_ref[:, count : 2 * count, :] = sent
            for k in range(CH):
                dweight_sum[pl.ds(k, CH, stride=CH), :] = flat[k * CH : (k + 1) * CH]

        @pl.when(term == 1)
        def _():
            send_ref[:, :count, :] = sent
            whole = (dweight_sum[...] + flat).astype(BF16)
            peers = send_ref.shape[0]
            end = 2 * count + whole.shape[0] // peers
            send_ref[:, 2 * count : end, :] = whole.reshape(peers, -1, whole.shape[1])
            d_bias = jnp.sum(dbias_acc[...], axis=0, keepdims=True)
            first = d_bias.astype(BF16).astype(F32)
            place = lax.broadcasted_iota(jnp.int32, (TILE, 128), 0)
            rows = jnp.where(place == 0, first, jnp.where(place == 1, d_bias - first, 0.0))
            for r in range(peers):
                send_ref[r, end : end + TILE, :] = rows.astype(BF16)


def lane_kernel(across, core_ref, grads_ref, row_ref, cols_ref, row_t):
    term, step = pl.program_id(0), pl.program_id(1)
    depth = CH // GROUP * across
    _, owners, height, _ = cols_ref.shape
    own = height // (2 * CH)
    core = core_ref[0]

    @pl.when(step == 0)
    def _():
        for m in range(GROUP):
            row_t[m] = row_ref[0, m * depth : (m + 1) * depth, :].T

    for n in range(0, BLOCK * CH, 256):
        d_lane = None
        for m in range(GROUP):
            wide = jnp.dot(
                row_t[m],
                from_tiles(grads_ref.at[0, 0], m, n // 128, 2),
                preferred_element_type=F32,
            )
            wide = unturned(wide, m)
            d_lane = wide if d_lane is None else d_lane + wide
        d_lane = (d_lane.T * (1.0 / SEQS)).astype(BF16)
        for r in range(256 // CH):
            residue = step * BLOCK + n // CH + r
            owner = residue // own
            place = (owner + core) % 2
            to_row = pl.multiple_of((term * own + residue % own) * CH, CH)
            cols_ref[place, owner // 2, pl.ds(to_row, CH), :] = d_lane[r * CH : (r + 1) * CH]


def lane_block(core, grads, rows, own):
    _, steps, _, groups, depth, _ = grads.shape
    across = depth // (CH // GROUP)
    owners = steps * BLOCK // own
    return pl.pallas_call(
        functools.partial(lane_kernel, across),
        grid=(2, steps),
        in_specs=[
            pl.BlockSpec(memory_space=pltpu.SMEM),
            pl.BlockSpec(
                (1, 1, GROUP, groups, depth, 128), lambda t, s: (t, s, 0, 0, 0, 0)
            ),
            pl.BlockSpec((1, CH * across, SEQS), lambda t, s: (t, 0, 0)),
        ],
        out_specs=pl.BlockSpec((2, owners // 2, 2 * own * CH, SEQS), lambda t, s: (0, 0, 0, 0)),
        out_shape=jax.ShapeDtypeStruct((2, owners // 2, 2 * own * CH, SEQS), BF16),
        scratch_shapes=[pltpu.VMEM((GROUP, SEQS, depth), BF16)],
        compiler_params=pltpu.CompilerParams(vmem_limit_bytes=40 * 1024 * 1024),
        cost_estimate=pl.CostEstimate(
            flops=4 * steps * BLOCK * across * CH * CH * SEQS,
            bytes_accessed=24 * 1024 * 1024,
            transcendentals=0,
        ),
    )(core, grads, rows)


def pair_block(lanes, rows, weights, bias, upstream, row_peers):
    count, across, pairs = upstream.shape
    steps = count // BLOCK
    width = BLOCK * CH
    depth = CH // GROUP * across
    once = lambda t, s: (0, 0)
    sent = 2 * CH * across // row_peers + CH * CH // row_peers + TILE
    return pl.pallas_call(
        functools.partial(pair_kernel, steps, across),
        grid=(2, steps),
        in_specs=[
            pl.BlockSpec((1, width, SEQS), lambda t, s: (t, s, 0)),
            pl.BlockSpec((1, CH * across, SEQS), lambda t, s: (t, 0, 0)),
            pl.BlockSpec((1, CH * CH, pairs), lambda t, s: (t, 0, 0)),
            pl.BlockSpec((1, pairs), once),
            pl.BlockSpec((BLOCK, across, pairs), lambda t, s: (s, 0, 0)),
        ],
        out_specs=[
            pl.BlockSpec((BLOCK, across, pairs), lambda t, s: (t * s, 0, 0)),
            pl.BlockSpec(
                (1, 1, GROUP, width // 128, depth, 128), lambda t, s: (t, s, 0, 0, 0, 0)
            ),
            pl.BlockSpec((row_peers, sent, SEQS), lambda t, s: (0, 0, 0)),
        ],
        out_shape=[
            jax.ShapeDtypeStruct((count, across, pairs), BF16),
            jax.ShapeDtypeStruct((2, steps, GROUP, width // 128, depth, 128), BF16),
            jax.ShapeDtypeStruct((row_peers, sent, SEQS), BF16),
        ],
        scratch_shapes=[
            pltpu.VMEM((count, across, pairs), F32),
            pltpu.VMEM((GROUP, width // 128, depth, 128), BF16),
            pltpu.VMEM((GROUP, width // 128, depth, 128), BF16),
            pltpu.VMEM((CH * across, SEQS), F32),
            pltpu.VMEM((GROUP, pairs, CH * CH), F32),
            pltpu.VMEM((CH * CH, pairs), F32),
            pltpu.VMEM((CH * across, SEQS), F32),
            pltpu.VMEM((8, pairs), F32),
        ],
        compiler_params=pltpu.CompilerParams(vmem_limit_bytes=60 * 1024 * 1024),
        cost_estimate=pl.CostEstimate(
            flops=10 * count * across * CH * CH * SEQS * 2,
            bytes_accessed=32 * 1024 * 1024,
            transcendentals=0,
        ),
    )(lanes, rows, weights, bias, upstream)


def exchange(x, axis, groups=None):
    return lax.all_to_all(
        x, axis, split_axis=0, concat_axis=0, axis_index_groups=groups, tiled=True
    )


def everywhere(x, axis, groups=None):
    members = lax.axis_size(axis) if groups is None else len(groups[0])
    copies = jnp.broadcast_to(x[None], (members,) + x.shape)
    return exchange(copies, axis, groups)


def two_parts(x):
    high = x.astype(BF16)
    low = (x - high.astype(F32)).astype(BF16)
    return jnp.concatenate([high, low, jnp.zeros((TILE - 2, x.shape[1]), BF16)], axis=0)


def one_part(x):
    return jnp.sum(x[:2], axis=0, keepdims=True)


def local(left_features, right_features, weight, bias, upstream):
    rows_n, cols_n = lax.axis_size("row"), lax.axis_size("col")
    own, pairs = left_features.shape[0], weight.shape[1]
    count, across = upstream.shape[0], upstream.shape[1]
    to_part = [(o, (o % rows_n) * cols_n + o // rows_n) for o in range(rows_n * cols_n)]
    to_owner = [(b, a) for a, b in to_part]
    both = ("row", "col")
    same_core = [list(range(k, cols_n, 2)) for k in range(2)]
    other_core = [(k, k ^ 1) for k in range(cols_n)]
    n_own = 2 * own * CH

    def channels_first(x):
        return x.reshape(own, SEQS, CH).transpose(0, 2, 1)

    mine = jnp.stack([channels_first(left_features), channels_first(right_features)])
    mine = mine.reshape(2, own * CH, SEQS)
    part = lax.ppermute(mine, both, to_part)
    half = everywhere(mine, "col", same_core)
    other = lax.ppermute(half, "col", other_core)
    rows = everywhere(part, "row")
    second = lax.axis_index("col") % 2 == 1
    lanes = jnp.stack(
        [jnp.where(second, other, half), jnp.where(second, half, other)], axis=1
    )
    lanes = lanes.transpose(2, 0, 1, 3, 4).reshape(2, count * CH, SEQS)
    rows = rows.reshape(rows_n, 2, own, CH // GROUP, GROUP, SEQS)
    rows = rows[:, ::-1].transpose(1, 4, 3, 0, 2, 5).reshape(2, CH * across, SEQS)
    weights = jnp.stack(
        [weight.reshape(CH, CH, pairs).transpose(1, 0, 2).reshape(CH * CH, pairs), weight]
    )
    pair_out, g_terms, to_rows = pair_block(
        lanes, rows, weights, bias.reshape(1, pairs), upstream, rows_n
    )
    n_slice = CH * CH // rows_n

    def with_bias(x):
        return jnp.concatenate(
            [x[:n_slice].astype(BF16), two_parts(one_part(x[n_slice:]))], axis=0
        )

    sent = exchange(to_rows, "row")
    core = (lax.axis_index("col") % 2).astype(jnp.int32).reshape(1)
    to_cols = lane_block(core, g_terms, rows, own)
    other = lax.ppermute(to_cols[1], "col", other_core)
    summed = jnp.sum(sent.astype(F32), axis=0)
    part_grads = lax.ppermute(summed[:n_own].astype(BF16), both, to_owner)
    shared = with_bias(summed[n_own:])
    shared_other = lax.ppermute(shared, "col", other_core)
    shared = with_bias(shared.astype(F32) + shared_other.astype(F32))
    to_cols = (to_cols[0].astype(F32) + other.astype(F32)).astype(BF16)
    shared = jnp.broadcast_to(shared[None], (cols_n // 2,) + shared.shape)
    sent = exchange(jnp.concatenate([to_cols, shared], axis=1), "col", same_core)
    summed = jnp.sum(sent.astype(F32), axis=0)
    grad_weight = everywhere(summed[n_own : n_own + n_slice], "row")
    grad_weight = grad_weight.reshape(CH * CH, pairs)
    grad_bias = one_part(summed[n_own + n_slice :]).reshape(pairs)
    grads = summed[:n_own] + part_grads.astype(F32)
    grads = grads.reshape(2, own, CH, SEQS).transpose(0, 1, 3, 2).reshape(2, own, SEQS * CH)
    grads = grads.astype(BF16)
    return pair_out, grads[0], grads[1], grad_weight, grad_bias


def solution(mesh):
    placed = (P(("row", "col"), None), P(("row", "col"), None), P(), P(), P("row", "col", None))
    return jax.shard_map(
        local,
        mesh=mesh,
        in_specs=placed,
        out_specs=(
            P("row", "col", None),
            P(("row", "col"), None),
            P(("row", "col"), None),
            P(),
            P(),
        ),
        check_vma=False,
    )
```

```python
import functools

import jax
import jax.numpy as jnp
from jax import lax
from jax.experimental import pallas as pl
from jax.experimental.pallas import tpu as pltpu
from jax.sharding import PartitionSpec as P


CH = 32
SEQS = 128
GROUP = 4
BLOCK = 48
TILE = 16
BF16 = jnp.bfloat16
F32 = jnp.float32


def contract(a, b, dims):
    numbers = (((dims[0],), (dims[1],)), ((), ()))
    return lax.dot_general(a, b, numbers, preferred_element_type=F32)


def spread(parts, odd, high):
    once = [jnp.where(odd, parts[(r + 1) % GROUP], parts[r]) for r in range(GROUP)]
    twice = [jnp.where(high, once[(r + 2) % GROUP], once[r]) for r in range(GROUP)]
    return [twice[-q % GROUP] for q in range(GROUP)]


def unturned(wide, turn):
    if turn == 0:
        return wide
    return jnp.concatenate(
        [
            pltpu.roll(wide[:, n * 128 : (n + 1) * 128], 128 - CH * turn, 1)
            for n in range(wide.shape[1] // 128)
        ],
        axis=1,
    )


def to_tiles(ref, at, wide):
    for n in range(wide.shape[1] // 128):
        ref[at, n] = wide[:, n * 128 : (n + 1) * 128]


def from_tiles(ref, at, first=0, count=None):
    count = ref.shape[1] if count is None else count
    return jnp.concatenate([ref[at, first + n] for n in range(count)], axis=1)


def pair_kernel(
    across,
    lane_ref,
    row_ref,
    weight_ref,
    bias_ref,
    up_ref,
    pair_ref,
    grads_ref,
    send_ref,
    squares,
    products,
    packed,
    g_packed,
    g_tiles,
    drow_acc,
    dweight_acc,
    dweight_sum,
    drow_turned,
    dbias_acc,
    sent_sems,
):
    term = pl.program_id(0)
    quarters = CH // GROUP
    groups = lane_ref.shape[1] // (CH * GROUP)
    depth = quarters * across
    scale = 1.0 / SEQS
    lane = lax.broadcasted_iota(jnp.int32, (TILE, 128), 1) // CH
    odd = (lane % 2).astype(F32).astype(BF16) > 0.5
    high = (lane // 2).astype(F32).astype(BF16) > 0.5

    def turned_lanes(m):
        return jnp.concatenate(
            [
                lane_ref[0, pl.ds((GROUP * g + (p - m) % GROUP) * CH, CH), :]
                for g in range(groups)
                for p in range(GROUP)
            ],
            axis=0,
        )

    def turned_weight(q):
        return jnp.concatenate(
            [
                weight_ref[0, pl.ds((GROUP * k + (p - q) % GROUP) * CH, CH), :]
                for k in range(quarters)
                for p in range(GROUP)
            ],
            axis=0,
        )

    for m in range(GROUP):
        outer = contract(row_ref[0, m * depth : (m + 1) * depth, :], turned_lanes(m), (1, 1))
        to_tiles(products, m, (outer * scale).astype(BF16))

    def by_pair(k, _):
        from_rows = pl.multiple_of(k * across, TILE)
        for g in range(groups):
            for t in range(0, across, TILE):
                parts = [
                    products[m, g, pl.ds(from_rows + t, TILE), :] for m in range(GROUP)
                ]
                for q, tile in enumerate(spread(parts, odd, high)):
                    packed[q, k, pl.ds(g * across + t, TILE), :] = tile
        return _

    lax.fori_loop(0, quarters, by_pair, 0)
    for q in range(GROUP):
        outer = from_tiles(packed, q)
        weight_q = turned_weight(q)
        pre = jnp.dot(outer, weight_q, preferred_element_type=F32) + bias_ref[...]
        active = jnp.maximum(pre, 0.0)
        squared = active * active
        up = jnp.concatenate([up_ref[GROUP * g + q] for g in range(groups)], axis=0)
        d_pre = (active * up.astype(F32)).astype(BF16)

        for g in range(groups):
            place = GROUP * g + q
            here = squared[g * across : (g + 1) * across]
            pair_ref[GROUP * g + q] = ((here + squares[place]) * 0.5).astype(BF16)
            squares[place] = here
        to_tiles(g_packed, q, contract(d_pre, weight_q, (1, 1)).astype(BF16))
        dweight_acc[q] = contract(d_pre, outer, (0, 0))
        d_bias = jnp.sum(d_pre.astype(F32).reshape(groups * across // 8, 8, 128), axis=0)
        dbias_acc[...] = d_bias + jnp.where((term == 0) & (q == 0), 0.0, dbias_acc[...])

    def g_copy(term, k):
        rows = pl.ds(pl.multiple_of(k * across, TILE), across)
        return pltpu.make_async_copy(
            g_tiles.at[term, :, :, rows, :], grads_ref.at[term, :, :, rows, :], sent_sems.at[term, k]
        )

    def by_channel(k, _):
        to_rows = pl.multiple_of(k * across, TILE)
        for g in range(groups):
            for t in range(0, across, TILE):
                parts = [
                    g_packed[q, k, pl.ds(g * across + t, TILE), :] for q in range(GROUP)
                ]
                for m, tile in enumerate(spread(parts, odd, high)):
                    g_tiles[term, m, g, pl.ds(to_rows + t, TILE), :] = tile
        g_copy(term, k).start()
        return _

    lax.fori_loop(0, quarters, by_channel, 0)

    for m in range(GROUP):
        tiles = from_tiles(g_tiles.at[term], m)
        drow_acc[pl.ds(m * depth, depth)] = jnp.dot(
            tiles, turned_lanes(m), preferred_element_type=F32
        )

    for m in range(GROUP):
        for k in range(quarters):
            block = drow_acc[pl.ds(m * depth + k * across, across), :]
            drow_turned[pl.ds(k * GROUP + m, across, stride=CH), :] = block * scale
    sent = drow_turned[...].astype(BF16).reshape(send_ref.shape[0], -1, SEQS)
    count = sent.shape[1]
    total = dweight_acc[0]
    for q in range(1, GROUP):
        total = total + unturned(dweight_acc[q], q)
    flat = total.T

    @pl.when(term == 0)
    def _():
        send_ref[:, count : 2 * count, :] = sent
        for k in range(CH):
            dweight_sum[pl.ds(k, CH, stride=CH), :] = flat[k * CH : (k + 1) * CH]

    @pl.when(term == 1)
    def _():
        send_ref[:, :count, :] = sent
        whole = (dweight_sum[...] + flat).astype(BF16)
        peers = send_ref.shape[0]
        end = 2 * count + whole.shape[0] // peers
        send_ref[:, 2 * count : end, :] = whole.reshape(peers, -1, whole.shape[1])
        d_bias = jnp.sum(dbias_acc[...], axis=0, keepdims=True)
        first = d_bias.astype(BF16).astype(F32)
        place = lax.broadcasted_iota(jnp.int32, (TILE, 128), 0)
        rows = jnp.where(place == 0, first, jnp.where(place == 1, d_bias - first, 0.0))
        for r in range(peers):
            send_ref[r, end : end + TILE, :] = rows.astype(BF16)

    @pl.when(term == 1)
    def _():
        for t in range(2):
            for k in range(quarters):
                g_copy(t, k).wait()


def lane_kernel(across, core_ref, grads_ref, row_ref, mine_ref, theirs_ref, cols_ref, row_t):
    term, step = pl.program_id(0), pl.program_id(1)
    depth = CH // GROUP * across
    _, owners, height, _ = cols_ref.shape
    own = height // (2 * CH)
    core = core_ref[0]

    @pl.when(step == 0)
    def _():
        for m in range(GROUP):
            row_t[m] = row_ref[0, m * depth : (m + 1) * depth, :].T

    for n in range(0, BLOCK * CH, 256):
        d_lane = None
        for m in range(GROUP):
            wide = jnp.dot(
                row_t[m],
                from_tiles(grads_ref.at[0], m, n // 128, 2),
                preferred_element_type=F32,
            )
            wide = unturned(wide, m)
            d_lane = wide if d_lane is None else d_lane + wide
        d_lane = (d_lane.T * (1.0 / SEQS)).astype(BF16)
        for r in range(256 // CH):
            residue = step * BLOCK + n // CH + r
            owner = residue // own
            place = (owner + core) % 2
            to_row = pl.multiple_of((term * own + residue % own) * CH, CH)
            cols_ref[place, owner // 2, pl.ds(to_row, CH), :] = d_lane[r * CH : (r + 1) * CH]

    @pl.when((term == 1) & (step == pl.num_programs(1) - 1))
    def _():
        mine_ref[:, : 2 * own * CH, :] = cols_ref[0]
        theirs_ref[...] = cols_ref[1]


def lane_block(core, grads, rows, own, height):
    _, _, groups, depth, _ = grads.shape
    across = depth // (CH // GROUP)
    steps = groups * GROUP // BLOCK
    owners = steps * BLOCK // own
    return pl.pallas_call(
        functools.partial(lane_kernel, across),
        grid=(2, steps),
        in_specs=[
            pl.BlockSpec(memory_space=pltpu.SMEM),
            pl.BlockSpec(
                (1, GROUP, BLOCK // GROUP, depth, 128), lambda t, s: (t, 0, s, 0, 0)
            ),
            pl.BlockSpec((1, CH * across, SEQS), lambda t, s: (1 - t, 0, 0)),
        ],
        out_specs=[
            pl.BlockSpec((owners // 2, height, SEQS), lambda t, s: (0, 0, 0)),
            pl.BlockSpec((owners // 2, 2 * own * CH, SEQS), lambda t, s: (0, 0, 0)),
        ],
        out_shape=[
            jax.ShapeDtypeStruct((owners // 2, height, SEQS), BF16),
            jax.ShapeDtypeStruct((owners // 2, 2 * own * CH, SEQS), BF16),
        ],
        scratch_shapes=[
            pltpu.VMEM((2, owners // 2, 2 * own * CH, SEQS), BF16),
            pltpu.VMEM((GROUP, SEQS, depth), BF16),
        ],
        compiler_params=pltpu.CompilerParams(vmem_limit_bytes=40 * 1024 * 1024),
        cost_estimate=pl.CostEstimate(
            flops=4 * steps * BLOCK * across * CH * CH * SEQS,
            bytes_accessed=24 * 1024 * 1024,
            transcendentals=0,
        ),
    )(core, grads, rows)


def pair_block(lanes, rows, weights, bias, upstream, row_peers):
    count, across, pairs = upstream.shape
    width = count * CH
    depth = CH // GROUP * across
    high = count // GROUP * across
    sent = 2 * CH * across // row_peers + CH * CH // row_peers + TILE
    return pl.pallas_call(
        functools.partial(pair_kernel, across),
        grid=(2,),
        in_specs=[
            pl.BlockSpec((1, width, SEQS), lambda t: (t, 0, 0)),
            pl.BlockSpec((1, CH * across, SEQS), lambda t: (1 - t, 0, 0)),
            pl.BlockSpec((1, CH * CH, pairs), lambda t: (t, 0, 0)),
            pl.BlockSpec((1, pairs), lambda t: (0, 0)),
            pl.BlockSpec((count, across, pairs), lambda t: (0, 0, 0)),
        ],
        out_specs=[
            pl.BlockSpec((count, across, pairs), lambda t: (0, 0, 0)),
            pl.BlockSpec(memory_space=pl.ANY),
            pl.BlockSpec((row_peers, sent, SEQS), lambda t: (0, 0, 0)),
        ],
        out_shape=[
            jax.ShapeDtypeStruct((count, across, pairs), BF16),
            jax.ShapeDtypeStruct((2, GROUP, width // 128, depth, 128), BF16),
            jax.ShapeDtypeStruct((row_peers, sent, SEQS), BF16),
        ],
        scratch_shapes=[
            pltpu.VMEM((count, across, pairs), F32),
            pltpu.VMEM((GROUP, width // 128, depth, 128), BF16),
            pltpu.VMEM((GROUP, CH // GROUP, high, 128), BF16),
            pltpu.VMEM((GROUP, CH // GROUP, high, 128), BF16),
            pltpu.VMEM((2, GROUP, width // 128, depth, 128), BF16),
            pltpu.VMEM((CH * across, SEQS), F32),
            pltpu.VMEM((GROUP, pairs, CH * CH), F32),
            pltpu.VMEM((CH * CH, pairs), F32),
            pltpu.VMEM((CH * across, SEQS), F32),
            pltpu.VMEM((8, pairs), F32),
            pltpu.SemaphoreType.DMA((2, CH // GROUP)),
        ],
        compiler_params=pltpu.CompilerParams(vmem_limit_bytes=60 * 1024 * 1024),
        cost_estimate=pl.CostEstimate(
            flops=10 * count * across * CH * CH * SEQS * 2,
            bytes_accessed=32 * 1024 * 1024,
            transcendentals=0,
        ),
    )(lanes, rows, weights, bias, upstream)


def exchange(x, axis, groups=None):
    return lax.all_to_all(
        x, axis, split_axis=0, concat_axis=0, axis_index_groups=groups, tiled=True
    )


def everywhere(x, axis, groups=None):
    members = lax.axis_size(axis) if groups is None else len(groups[0])
    copies = jnp.broadcast_to(x[None], (members,) + x.shape)
    return exchange(copies, axis, groups)


def two_parts(x):
    high = x.astype(BF16)
    low = (x - high.astype(F32)).astype(BF16)
    return jnp.concatenate([high, low, jnp.zeros((TILE - 2, x.shape[1]), BF16)], axis=0)


def one_part(x):
    return jnp.sum(x[:2], axis=0, keepdims=True)


def local(left_features, right_features, weight, bias, upstream):
    rows_n, cols_n = lax.axis_size("row"), lax.axis_size("col")
    own, pairs = left_features.shape[0], weight.shape[1]
    count, across = upstream.shape[0], upstream.shape[1]
    to_part = [(o, (o % rows_n) * cols_n + o // rows_n) for o in range(rows_n * cols_n)]
    to_owner = [(b, a) for a, b in to_part]
    both = ("row", "col")
    same_core = [list(range(k, cols_n, 2)) for k in range(2)]
    other_core = [(k, k ^ 1) for k in range(cols_n)]
    n_own = 2 * own * CH

    def channels_first(x):
        return x.reshape(own, SEQS, CH).transpose(0, 2, 1)

    mine = jnp.stack([channels_first(left_features), channels_first(right_features)])
    mine = mine.reshape(2, own * CH, SEQS)
    part = lax.ppermute(mine, both, to_part)
    half = everywhere(mine, "col", same_core)
    other = lax.ppermute(half, "col", other_core)
    rows = everywhere(part, "row")
    second = (lax.axis_index("col") & 1) == 1
    lanes = jnp.stack([jnp.where(second, other, half), jnp.where(second, half, other)], axis=1)
    lanes = lanes.transpose(2, 0, 1, 3, 4).reshape(2, count * CH, SEQS)
    rows = rows.reshape(rows_n, 2, own, CH // GROUP, GROUP, SEQS)
    rows = rows.transpose(1, 4, 3, 0, 2, 5).reshape(2, CH * across, SEQS)
    weights = jnp.stack(
        [weight.reshape(CH, CH, pairs).transpose(1, 0, 2).reshape(CH * CH, pairs), weight]
    )
    pair_out, g_terms, to_rows = pair_block(
        lanes, rows, weights, bias.reshape(1, pairs), upstream, rows_n
    )
    n_slice = CH * CH // rows_n

    def with_bias(x):
        return jnp.concatenate(
            [x[:n_slice].astype(BF16), two_parts(one_part(x[n_slice:]))], axis=0
        )

    sent = exchange(to_rows, "row")
    core = (lax.axis_index("col") & 1).astype(jnp.int32).reshape(1)
    to_cols, theirs = lane_block(core, g_terms, rows, own, n_own + n_slice + TILE)
    other = lax.ppermute(theirs, "col", other_core)
    summed = jnp.sum(sent.astype(F32), axis=0)
    part_grads = lax.ppermute(summed[:n_own].astype(BF16), both, to_owner)
    shared = with_bias(summed[n_own:])
    shared_other = lax.ppermute(shared, "col", other_core)
    shared = with_bias(shared.astype(F32) + shared_other.astype(F32))
    mine = (to_cols[:, :n_own].astype(F32) + other.astype(F32)).astype(BF16)
    to_cols = lax.dynamic_update_slice(to_cols, mine, (0, 0, 0))
    shared = jnp.broadcast_to(shared[None], (cols_n // 2,) + shared.shape)
    to_cols = lax.dynamic_update_slice(to_cols, shared, (0, n_own, 0))
    sent = exchange(to_cols, "col", same_core)
    summed = jnp.sum(sent.astype(F32), axis=0)
    grad_weight = everywhere(summed[n_own : n_own + n_slice].astype(BF16), "row")
    grad_weight = grad_weight.astype(F32).reshape(CH * CH, pairs)
    grad_bias = one_part(summed[n_own + n_slice :]).reshape(pairs)
    grads = summed[:n_own] + part_grads.astype(F32)
    grads = grads.reshape(2, own, CH, SEQS).transpose(0, 1, 3, 2).reshape(2, own, SEQS * CH)
    grads = grads.astype(BF16)
    return pair_out, grads[0], grads[1], grad_weight, grad_bias


def solution(mesh):
    placed = (P(("row", "col"), None), P(("row", "col"), None), P(), P(), P("row", "col", None))
    return jax.shard_map(
        local,
        mesh=mesh,
        in_specs=placed,
        out_specs=(
            P("row", "col", None),
            P(("row", "col"), None),
            P(("row", "col"), None),
            P(),
            P(),
        ),
        check_vma=False,
    )
```

```python
import functools

import jax
import jax.numpy as jnp
from jax import lax
from jax.experimental import pallas as pl
from jax.experimental.pallas import tpu as pltpu
from jax.sharding import PartitionSpec as P


CH = 32
SEQS = 128
GROUP = 4
BLOCK = 48
TILE = 16
BF16 = jnp.bfloat16
F32 = jnp.float32


def contract(a, b, dims):
    numbers = (((dims[0],), (dims[1],)), ((), ()))
    return lax.dot_general(a, b, numbers, preferred_element_type=F32)


def spread(parts, odd, high):
    once = [jnp.where(odd, parts[(r + 1) % GROUP], parts[r]) for r in range(GROUP)]
    twice = [jnp.where(high, once[(r + 2) % GROUP], once[r]) for r in range(GROUP)]
    return [twice[-q % GROUP] for q in range(GROUP)]


def unturned(wide, turn):
    if turn == 0:
        return wide
    return jnp.concatenate(
        [
            pltpu.roll(wide[:, n * 128 : (n + 1) * 128], 128 - CH * turn, 1)
            for n in range(wide.shape[1] // 128)
        ],
        axis=1,
    )


def to_tiles(ref, at, wide):
    for n in range(wide.shape[1] // 128):
        ref[at, n] = wide[:, n * 128 : (n + 1) * 128]


def from_tiles(ref, at, first=0, count=None):
    count = ref.shape[1] if count is None else count
    return jnp.concatenate([ref[at, first + n] for n in range(count)], axis=1)


def pair_kernel(
    across,
    lane_ref,
    row_ref,
    weight_ref,
    bias_ref,
    up_ref,
    pair_ref,
    grads_ref,
    send_ref,
    squares,
    products,
    packed,
    g_packed,
    g_tiles,
    drow_acc,
    dweight_acc,
    dweight_sum,
    drow_turned,
    dbias_acc,
    sent_sems,
):
    term = pl.program_id(0)
    quarters = CH // GROUP
    groups = lane_ref.shape[1] // (CH * GROUP)
    depth = quarters * across
    scale = 1.0 / SEQS
    lane = lax.broadcasted_iota(jnp.int32, (TILE, 128), 1) // CH
    odd = (lane % 2).astype(F32).astype(BF16) > 0.5
    high = (lane // 2).astype(F32).astype(BF16) > 0.5

    def turned_lanes(m):
        return jnp.concatenate(
            [
                lane_ref[0, pl.ds((GROUP * g + (p - m) % GROUP) * CH, CH), :]
                for g in range(groups)
                for p in range(GROUP)
            ],
            axis=0,
        )

    def turned_weight(q):
        return jnp.concatenate(
            [
                weight_ref[0, pl.ds((GROUP * k + (p - q) % GROUP) * CH, CH), :]
                for k in range(quarters)
                for p in range(GROUP)
            ],
            axis=0,
        )

    for m in range(GROUP):
        outer = contract(row_ref[0, m * depth : (m + 1) * depth, :], turned_lanes(m), (1, 1))
        to_tiles(products, m, (outer * scale).astype(BF16))

    def by_pair(k, _):
        from_rows = pl.multiple_of(k * across, TILE)
        for g in range(groups):
            for t in range(0, across, TILE):
                parts = [
                    products[m, g, pl.ds(from_rows + t, TILE), :] for m in range(GROUP)
                ]
                for q, tile in enumerate(spread(parts, odd, high)):
                    packed[q, k, pl.ds(g * across + t, TILE), :] = tile
        return _

    lax.fori_loop(0, quarters, by_pair, 0)
    for q in range(GROUP):
        outer = from_tiles(packed, q)
        weight_q = turned_weight(q)
        pre = jnp.dot(outer, weight_q, preferred_element_type=F32) + bias_ref[...]
        active = jnp.maximum(pre, 0.0)
        squared = active * active
        up = jnp.concatenate([up_ref[GROUP * g + q] for g in range(groups)], axis=0)
        d_pre = (active * up.astype(F32)).astype(BF16)

        for g in range(groups):
            place = GROUP * g + q
            here = squared[g * across : (g + 1) * across]
            pair_ref[GROUP * g + q] = ((here + squares[place]) * 0.5).astype(BF16)
            squares[place] = here
        to_tiles(g_packed, q, contract(d_pre, weight_q, (1, 1)).astype(BF16))
        dweight_acc[q] = contract(d_pre, outer, (0, 0))
        d_bias = jnp.sum(d_pre.astype(F32).reshape(groups * across // 8, 8, 128), axis=0)
        dbias_acc[...] = d_bias + jnp.where((term == 0) & (q == 0), 0.0, dbias_acc[...])

    def g_copy(term, k):
        rows = pl.ds(pl.multiple_of(k * across, TILE), across)
        return pltpu.make_async_copy(
            g_tiles.at[term, :, :, rows, :], grads_ref.at[term, :, :, rows, :], sent_sems.at[term, k]
        )

    def by_channel(k, _):
        to_rows = pl.multiple_of(k * across, TILE)
        for g in range(groups):
            for t in range(0, across, TILE):
                parts = [
                    g_packed[q, k, pl.ds(g * across + t, TILE), :] for q in range(GROUP)
                ]
                for m, tile in enumerate(spread(parts, odd, high)):
                    g_tiles[term, m, g, pl.ds(to_rows + t, TILE), :] = tile
        g_copy(term, k).start()
        return _

    lax.fori_loop(0, quarters, by_channel, 0)

    for m in range(GROUP):
        tiles = from_tiles(g_tiles.at[term], m)
        drow_acc[pl.ds(m * depth, depth)] = jnp.dot(
            tiles, turned_lanes(m), preferred_element_type=F32
        )

    for m in range(GROUP):
        for k in range(quarters):
            block = drow_acc[pl.ds(m * depth + k * across, across), :]
            drow_turned[pl.ds(k * GROUP + m, across, stride=CH), :] = block * scale
    sent = drow_turned[...].astype(BF16).reshape(send_ref.shape[0], -1, SEQS)
    count = sent.shape[1]
    total = dweight_acc[0]
    for q in range(1, GROUP):
        total = total + unturned(dweight_acc[q], q)
    flat = total.T

    @pl.when(term == 0)
    def _():
        send_ref[:, count : 2 * count, :] = sent
        for k in range(CH):
            dweight_sum[pl.ds(k, CH, stride=CH), :] = flat[k * CH : (k + 1) * CH]

    @pl.when(term == 1)
    def _():
        send_ref[:, :count, :] = sent
        whole = (dweight_sum[...] + flat).astype(BF16)
        peers = send_ref.shape[0]
        end = 2 * count + whole.shape[0] // peers
        send_ref[:, 2 * count : end, :] = whole.reshape(peers, -1, whole.shape[1])
        d_bias = jnp.sum(dbias_acc[...], axis=0, keepdims=True)
        first = d_bias.astype(BF16).astype(F32)
        place = lax.broadcasted_iota(jnp.int32, (TILE, 128), 0)
        rows = jnp.where(place == 0, first, jnp.where(place == 1, d_bias - first, 0.0))
        for r in range(peers):
            send_ref[r, end : end + TILE, :] = rows.astype(BF16)

    @pl.when(term == 1)
    def _():
        for t in range(2):
            for k in range(quarters):
                g_copy(t, k).wait()


def lane_kernel(across, core_ref, grads_ref, row_ref, mine_ref, theirs_ref, cols_ref, row_t):
    term, step = pl.program_id(0), pl.program_id(1)
    depth = CH // GROUP * across
    _, owners, height, _ = cols_ref.shape
    own = height // (2 * CH)
    core = core_ref[0]

    @pl.when(step == 0)
    def _():
        for m in range(GROUP):
            row_t[m] = row_ref[0, m * depth : (m + 1) * depth, :].T

    for n in range(0, BLOCK * CH, 256):
        d_lane = None
        for m in range(GROUP):
            wide = jnp.dot(
                row_t[m],
                from_tiles(grads_ref.at[0], m, n // 128, 2),
                preferred_element_type=F32,
            )
            wide = unturned(wide, m)
            d_lane = wide if d_lane is None else d_lane + wide
        d_lane = (d_lane.T * (1.0 / SEQS)).astype(BF16)
        for r in range(256 // CH):
            residue = step * BLOCK + n // CH + r
            owner = residue // own
            place = (owner + core) % 2
            to_row = pl.multiple_of((term * own + residue % own) * CH, CH)
            cols_ref[place, owner // 2, pl.ds(to_row, CH), :] = d_lane[r * CH : (r + 1) * CH]

    @pl.when((term == 1) & (step == pl.num_programs(1) - 1))
    def _():
        mine_ref[:, : 2 * own * CH, :] = cols_ref[0]
        theirs_ref[...] = cols_ref[1]


def lane_block(core, grads, rows, own, height):
    _, _, groups, depth, _ = grads.shape
    across = depth // (CH // GROUP)
    steps = groups * GROUP // BLOCK
    owners = steps * BLOCK // own
    return pl.pallas_call(
        functools.partial(lane_kernel, across),
        grid=(2, steps),
        in_specs=[
            pl.BlockSpec(memory_space=pltpu.SMEM),
            pl.BlockSpec(
                (1, GROUP, BLOCK // GROUP, depth, 128), lambda t, s: (t, 0, s, 0, 0)
            ),
            pl.BlockSpec((1, CH * across, SEQS), lambda t, s: (1 - t, 0, 0)),
        ],
        out_specs=[
            pl.BlockSpec((owners // 2, height, SEQS), lambda t, s: (0, 0, 0)),
            pl.BlockSpec((owners // 2, 2 * own * CH, SEQS), lambda t, s: (0, 0, 0)),
        ],
        out_shape=[
            jax.ShapeDtypeStruct((owners // 2, height, SEQS), BF16),
            jax.ShapeDtypeStruct((owners // 2, 2 * own * CH, SEQS), BF16),
        ],
        scratch_shapes=[
            pltpu.VMEM((2, owners // 2, 2 * own * CH, SEQS), BF16),
            pltpu.VMEM((GROUP, SEQS, depth), BF16),
        ],
        compiler_params=pltpu.CompilerParams(vmem_limit_bytes=40 * 1024 * 1024),
        cost_estimate=pl.CostEstimate(
            flops=4 * steps * BLOCK * across * CH * CH * SEQS,
            bytes_accessed=24 * 1024 * 1024,
            transcendentals=0,
        ),
    )(core, grads, rows)


def pair_block(lanes, rows, weights, bias, upstream, row_peers):
    count, across, pairs = upstream.shape
    width = count * CH
    depth = CH // GROUP * across
    high = count // GROUP * across
    sent = 2 * CH * across // row_peers + CH * CH // row_peers + TILE
    return pl.pallas_call(
        functools.partial(pair_kernel, across),
        grid=(2,),
        in_specs=[
            pl.BlockSpec((1, width, SEQS), lambda t: (t, 0, 0)),
            pl.BlockSpec((1, CH * across, SEQS), lambda t: (1 - t, 0, 0)),
            pl.BlockSpec((1, CH * CH, pairs), lambda t: (t, 0, 0)),
            pl.BlockSpec((1, pairs), lambda t: (0, 0)),
            pl.BlockSpec((count, across, pairs), lambda t: (0, 0, 0)),
        ],
        out_specs=[
            pl.BlockSpec((count, across, pairs), lambda t: (0, 0, 0)),
            pl.BlockSpec(memory_space=pl.ANY),
            pl.BlockSpec((row_peers, sent, SEQS), lambda t: (0, 0, 0)),
        ],
        out_shape=[
            jax.ShapeDtypeStruct((count, across, pairs), BF16),
            jax.ShapeDtypeStruct((2, GROUP, width // 128, depth, 128), BF16),
            jax.ShapeDtypeStruct((row_peers, sent, SEQS), BF16),
        ],
        scratch_shapes=[
            pltpu.VMEM((count, across, pairs), F32),
            pltpu.VMEM((GROUP, width // 128, depth, 128), BF16),
            pltpu.VMEM((GROUP, CH // GROUP, high, 128), BF16),
            pltpu.VMEM((GROUP, CH // GROUP, high, 128), BF16),
            pltpu.VMEM((2, GROUP, width // 128, depth, 128), BF16),
            pltpu.VMEM((CH * across, SEQS), F32),
            pltpu.VMEM((GROUP, pairs, CH * CH), F32),
            pltpu.VMEM((CH * CH, pairs), F32),
            pltpu.VMEM((CH * across, SEQS), F32),
            pltpu.VMEM((8, pairs), F32),
            pltpu.SemaphoreType.DMA((2, CH // GROUP)),
        ],
        compiler_params=pltpu.CompilerParams(vmem_limit_bytes=60 * 1024 * 1024),
        cost_estimate=pl.CostEstimate(
            flops=10 * count * across * CH * CH * SEQS * 2,
            bytes_accessed=32 * 1024 * 1024,
            transcendentals=0,
        ),
    )(lanes, rows, weights, bias, upstream)


def exchange(x, axis, groups=None):
    return lax.all_to_all(
        x, axis, split_axis=0, concat_axis=0, axis_index_groups=groups, tiled=True
    )


def everywhere(x, axis, groups=None):
    members = lax.axis_size(axis) if groups is None else len(groups[0])
    copies = jnp.broadcast_to(x[None], (members,) + x.shape)
    return exchange(copies, axis, groups)


def two_parts(x):
    high = x.astype(BF16)
    low = (x - high.astype(F32)).astype(BF16)
    return jnp.concatenate([high, low, jnp.zeros((TILE - 2, x.shape[1]), BF16)], axis=0)


def one_part(x):
    return jnp.sum(x[:2], axis=0, keepdims=True)


def local(left_features, right_features, weight, bias, upstream):
    rows_n, cols_n = lax.axis_size("row"), lax.axis_size("col")
    own, pairs = left_features.shape[0], weight.shape[1]
    count, across = upstream.shape[0], upstream.shape[1]
    to_part = [(o, (o % rows_n) * cols_n + o // rows_n) for o in range(rows_n * cols_n)]
    to_owner = [(b, a) for a, b in to_part]
    both = ("row", "col")
    same_core = [list(range(k, cols_n, 2)) for k in range(2)]
    other_core = [(k, k ^ 1) for k in range(cols_n)]
    n_own = 2 * own * CH

    mine = jnp.concatenate([left_features, right_features], axis=0)
    mine = mine.reshape(2 * own, SEQS, CH).transpose(0, 2, 1).reshape(2, own * CH, SEQS)
    turned = weight.reshape(CH, CH, pairs).transpose(1, 0, 2).reshape(CH * CH, pairs)
    weights = jnp.stack([turned, weight])
    part = lax.ppermute(mine, both, to_part)
    half = everywhere(mine, "col", same_core)
    other = lax.ppermute(half, "col", other_core)
    rows = everywhere(part, "row")
    second = (lax.axis_index("col") & 1) == 1
    lanes = jnp.stack([jnp.where(second, other, half), jnp.where(second, half, other)], axis=1)
    lanes = lanes.transpose(2, 0, 1, 3, 4).reshape(2, count * CH, SEQS)
    rows = rows.reshape(rows_n, 2, own, CH // GROUP, GROUP, SEQS)
    rows = rows.transpose(1, 4, 3, 0, 2, 5).reshape(2, CH * across, SEQS)
    pair_out, g_terms, to_rows = pair_block(
        lanes, rows, weights, bias.reshape(1, pairs), upstream, rows_n
    )
    n_slice = CH * CH // rows_n

    def with_bias(x):
        return jnp.concatenate(
            [x[:n_slice].astype(BF16), two_parts(one_part(x[n_slice:]))], axis=0
        )

    sent = exchange(to_rows, "row")
    core = (lax.axis_index("col") & 1).astype(jnp.int32).reshape(1)
    to_cols, theirs = lane_block(core, g_terms, rows, own, n_own)
    other = lax.ppermute(theirs, "col", other_core)
    summed = jnp.sum(sent.astype(F32), axis=0)
    part_grads = lax.ppermute(summed[:n_own].astype(BF16), both, to_owner)
    shared = with_bias(summed[n_own:])
    shared_other = lax.ppermute(shared, "col", other_core)
    shared = with_bias(shared.astype(F32) + shared_other.astype(F32))
    mine = (to_cols[:, :n_own].astype(F32) + other.astype(F32)).astype(BF16)
    shared = jnp.broadcast_to(shared[None], (cols_n // 2,) + shared.shape)
    sent = exchange(jnp.concatenate([mine, shared], axis=1), "col", same_core)
    summed = jnp.sum(sent.astype(F32), axis=0)
    grad_weight = everywhere(summed[n_own : n_own + n_slice].astype(BF16), "row")
    grad_weight = grad_weight.astype(F32).reshape(CH * CH, pairs)
    grad_bias = one_part(summed[n_own + n_slice :]).reshape(pairs)
    grads = summed[:n_own] + part_grads.astype(F32)
    grads = grads.reshape(2, own, CH, SEQS).transpose(0, 1, 3, 2).reshape(2, own, SEQS * CH)
    grads = grads.astype(BF16)
    return pair_out, grads[0], grads[1], grad_weight, grad_bias


def solution(mesh):
    placed = (P(("row", "col"), None), P(("row", "col"), None), P(), P(), P("row", "col", None))
    return jax.shard_map(
        local,
        mesh=mesh,
        in_specs=placed,
        out_specs=(
            P("row", "col", None),
            P(("row", "col"), None),
            P(("row", "col"), None),
            P(),
            P(),
        ),
        check_vma=False,
    )
```

```python
import functools

import jax
import jax.numpy as jnp
from jax import lax
from jax.experimental import pallas as pl
from jax.experimental.pallas import tpu as pltpu
from jax.sharding import PartitionSpec as P


CH = 32
SEQS = 128
GROUP = 4
BLOCK = 48
TILE = 16
BF16 = jnp.bfloat16
F32 = jnp.float32


def contract(a, b, dims):
    numbers = (((dims[0],), (dims[1],)), ((), ()))
    return lax.dot_general(a, b, numbers, preferred_element_type=F32)


def spread(parts, odd, high):
    once = [jnp.where(odd, parts[(r + 1) % GROUP], parts[r]) for r in range(GROUP)]
    twice = [jnp.where(high, once[(r + 2) % GROUP], once[r]) for r in range(GROUP)]
    return [twice[-q % GROUP] for q in range(GROUP)]


def unturned(wide, turn):
    if turn == 0:
        return wide
    return jnp.concatenate(
        [
            pltpu.roll(wide[:, n * 128 : (n + 1) * 128], 128 - CH * turn, 1)
            for n in range(wide.shape[1] // 128)
        ],
        axis=1,
    )


def to_tiles(ref, at, wide):
    for n in range(wide.shape[1] // 128):
        ref[at, n] = wide[:, n * 128 : (n + 1) * 128]


def from_tiles(ref, at, first=0, count=None):
    count = ref.shape[1] if count is None else count
    return jnp.concatenate([ref[at, first + n] for n in range(count)], axis=1)


def pair_kernel(
    across,
    lane_ref,
    row_ref,
    weight_ref,
    bias_ref,
    up_ref,
    pair_ref,
    grads_ref,
    send_ref,
    squares,
    products,
    packed,
    g_packed,
    g_tiles,
    drow_acc,
    dweight_acc,
    dweight_sum,
    dbias_acc,
    sent_sems,
):
    term = pl.program_id(0)
    quarters = CH // GROUP
    groups = lane_ref.shape[1] // (CH * GROUP)
    depth = quarters * across
    scale = 1.0 / SEQS
    lane = lax.broadcasted_iota(jnp.int32, (TILE, 128), 1) // CH
    odd = (lane % 2).astype(F32).astype(BF16) > 0.5
    high = (lane // 2).astype(F32).astype(BF16) > 0.5

    def turned_lanes(m):
        return jnp.concatenate(
            [
                lane_ref[0, pl.ds((GROUP * g + (p - m) % GROUP) * CH, CH), :]
                for g in range(groups)
                for p in range(GROUP)
            ],
            axis=0,
        )

    def turned_weight(q):
        return jnp.concatenate(
            [
                weight_ref[0, pl.ds((GROUP * k + (p - q) % GROUP) * CH, CH), :]
                for k in range(quarters)
                for p in range(GROUP)
            ],
            axis=0,
        )

    for m in range(GROUP):
        outer = contract(row_ref[0, m * depth : (m + 1) * depth, :], turned_lanes(m), (1, 1))
        to_tiles(products, m, (outer * scale).astype(BF16))

    def by_pair(k, _):
        from_rows = pl.multiple_of(k * across, TILE)
        for g in range(groups):
            for t in range(0, across, TILE):
                parts = [
                    products[m, g, pl.ds(from_rows + t, TILE), :] for m in range(GROUP)
                ]
                for q, tile in enumerate(spread(parts, odd, high)):
                    packed[q, k, pl.ds(g * across + t, TILE), :] = tile
        return _

    lax.fori_loop(0, quarters, by_pair, 0)
    for q in range(GROUP):
        outer = from_tiles(packed, q)
        weight_q = turned_weight(q)
        pre = jnp.dot(outer, weight_q, preferred_element_type=F32) + bias_ref[...]
        active = jnp.maximum(pre, 0.0)
        squared = active * active
        up = jnp.concatenate([up_ref[GROUP * g + q] for g in range(groups)], axis=0)
        d_pre = (active * up.astype(F32)).astype(BF16)

        for g in range(groups):
            place = GROUP * g + q
            here = squared[g * across : (g + 1) * across]
            pair_ref[GROUP * g + q] = ((here + squares[place]) * 0.5).astype(BF16)
            squares[place] = here
        to_tiles(g_packed, q, contract(d_pre, weight_q, (1, 1)).astype(BF16))
        dweight_acc[q] = contract(d_pre, outer, (0, 0))
        d_bias = jnp.sum(d_pre.astype(F32).reshape(groups * across // 8, 8, 128), axis=0)
        dbias_acc[...] = d_bias + jnp.where((term == 0) & (q == 0), 0.0, dbias_acc[...])

    def g_copy(term, k):
        rows = pl.ds(pl.multiple_of(k * across, TILE), across)
        return pltpu.make_async_copy(
            g_tiles.at[term, :, :, rows, :], grads_ref.at[term, :, :, rows, :], sent_sems.at[term, k]
        )

    def by_channel(k, _):
        to_rows = pl.multiple_of(k * across, TILE)
        for g in range(groups):
            for t in range(0, across, TILE):
                parts = [
                    g_packed[q, k, pl.ds(g * across + t, TILE), :] for q in range(GROUP)
                ]
                for m, tile in enumerate(spread(parts, odd, high)):
                    g_tiles[term, m, g, pl.ds(to_rows + t, TILE), :] = tile
        g_copy(term, k).start()
        return _

    lax.fori_loop(0, quarters, by_channel, 0)

    for m in range(GROUP):
        tiles = from_tiles(g_tiles.at[term], m)
        drow_acc[pl.ds(m * depth, depth)] = jnp.dot(
            tiles, turned_lanes(m), preferred_element_type=F32
        )

    by_channel_rows = jnp.stack(
        [
            drow_acc[pl.ds(m * depth + k * across, across), :]
            for k in range(quarters)
            for m in range(GROUP)
        ]
    )
    sent = (jnp.swapaxes(by_channel_rows, 0, 1) * scale).astype(BF16)
    sent = sent.reshape(send_ref.shape[0], -1, SEQS)
    count = sent.shape[1]
    total = dweight_acc[0]
    for q in range(1, GROUP):
        total = total + unturned(dweight_acc[q], q)
    flat = total.T

    @pl.when(term == 0)
    def _():
        send_ref[:, count : 2 * count, :] = sent
        dweight_sum[...] = jnp.swapaxes(flat.reshape(CH, CH, -1), 0, 1).reshape(flat.shape)

    @pl.when(term == 1)
    def _():
        send_ref[:, :count, :] = sent
        whole = (dweight_sum[...] + flat).astype(BF16)
        peers = send_ref.shape[0]
        end = 2 * count + whole.shape[0] // peers
        send_ref[:, 2 * count : end, :] = whole.reshape(peers, -1, whole.shape[1])
        d_bias = jnp.sum(dbias_acc[...], axis=0, keepdims=True)
        first = d_bias.astype(BF16).astype(F32)
        place = lax.broadcasted_iota(jnp.int32, (TILE, 128), 0)
        rows = jnp.where(place == 0, first, jnp.where(place == 1, d_bias - first, 0.0))
        for r in range(peers):
            send_ref[r, end : end + TILE, :] = rows.astype(BF16)

    @pl.when(term == 1)
    def _():
        for t in range(2):
            for k in range(quarters):
                g_copy(t, k).wait()


def lane_kernel(across, core_ref, grads_ref, row_ref, mine_ref, theirs_ref, cols_ref, row_t):
    term, step = pl.program_id(0), pl.program_id(1)
    depth = CH // GROUP * across
    _, owners, height, _ = cols_ref.shape
    own = height // (2 * CH)
    core = core_ref[0]

    @pl.when(step == 0)
    def _():
        for m in range(GROUP):
            row_t[m] = row_ref[0, m * depth : (m + 1) * depth, :].T

    for n in range(0, BLOCK * CH, 256):
        d_lane = None
        for m in range(GROUP):
            wide = jnp.dot(
                row_t[m],
                from_tiles(grads_ref.at[0], m, n // 128, 2),
                preferred_element_type=F32,
            )
            wide = unturned(wide, m)
            d_lane = wide if d_lane is None else d_lane + wide
        d_lane = (d_lane.T * (1.0 / SEQS)).astype(BF16)
        for r in range(256 // CH):
            residue = step * BLOCK + n // CH + r
            owner = residue // own
            place = (owner + core) % 2
            to_row = pl.multiple_of((term * own + residue % own) * CH, CH)
            cols_ref[place, owner // 2, pl.ds(to_row, CH), :] = d_lane[r * CH : (r + 1) * CH]

    @pl.when((term == 1) & (step == pl.num_programs(1) - 1))
    def _():
        mine_ref[:, : 2 * own * CH, :] = cols_ref[0]
        theirs_ref[...] = cols_ref[1]


def lane_block(core, grads, rows, own, height):
    _, _, groups, depth, _ = grads.shape
    across = depth // (CH // GROUP)
    steps = groups * GROUP // BLOCK
    owners = steps * BLOCK // own
    return pl.pallas_call(
        functools.partial(lane_kernel, across),
        grid=(2, steps),
        in_specs=[
            pl.BlockSpec(memory_space=pltpu.SMEM),
            pl.BlockSpec(
                (1, GROUP, BLOCK // GROUP, depth, 128), lambda t, s: (t, 0, s, 0, 0)
            ),
            pl.BlockSpec((1, CH * across, SEQS), lambda t, s: (1 - t, 0, 0)),
        ],
        out_specs=[
            pl.BlockSpec((owners // 2, height, SEQS), lambda t, s: (0, 0, 0)),
            pl.BlockSpec((owners // 2, 2 * own * CH, SEQS), lambda t, s: (0, 0, 0)),
        ],
        out_shape=[
            jax.ShapeDtypeStruct((owners // 2, height, SEQS), BF16),
            jax.ShapeDtypeStruct((owners // 2, 2 * own * CH, SEQS), BF16),
        ],
        scratch_shapes=[
            pltpu.VMEM((2, owners // 2, 2 * own * CH, SEQS), BF16),
            pltpu.VMEM((GROUP, SEQS, depth), BF16),
        ],
        compiler_params=pltpu.CompilerParams(vmem_limit_bytes=40 * 1024 * 1024),
        cost_estimate=pl.CostEstimate(
            flops=4 * steps * BLOCK * across * CH * CH * SEQS,
            bytes_accessed=24 * 1024 * 1024,
            transcendentals=0,
        ),
    )(core, grads, rows)


def pair_block(lanes, rows, weights, bias, upstream, row_peers):
    count, across, pairs = upstream.shape
    width = count * CH
    depth = CH // GROUP * across
    high = count // GROUP * across
    sent = 2 * CH * across // row_peers + CH * CH // row_peers + TILE
    return pl.pallas_call(
        functools.partial(pair_kernel, across),
        grid=(2,),
        in_specs=[
            pl.BlockSpec((1, width, SEQS), lambda t: (t, 0, 0)),
            pl.BlockSpec((1, CH * across, SEQS), lambda t: (1 - t, 0, 0)),
            pl.BlockSpec((1, CH * CH, pairs), lambda t: (t, 0, 0)),
            pl.BlockSpec((1, pairs), lambda t: (0, 0)),
            pl.BlockSpec((count, across, pairs), lambda t: (0, 0, 0)),
        ],
        out_specs=[
            pl.BlockSpec((count, across, pairs), lambda t: (0, 0, 0)),
            pl.BlockSpec(memory_space=pl.ANY),
            pl.BlockSpec((row_peers, sent, SEQS), lambda t: (0, 0, 0)),
        ],
        out_shape=[
            jax.ShapeDtypeStruct((count, across, pairs), BF16),
            jax.ShapeDtypeStruct((2, GROUP, width // 128, depth, 128), BF16),
            jax.ShapeDtypeStruct((row_peers, sent, SEQS), BF16),
        ],
        scratch_shapes=[
            pltpu.VMEM((count, across, pairs), F32),
            pltpu.VMEM((GROUP, width // 128, depth, 128), BF16),
            pltpu.VMEM((GROUP, CH // GROUP, high, 128), BF16),
            pltpu.VMEM((GROUP, CH // GROUP, high, 128), BF16),
            pltpu.VMEM((2, GROUP, width // 128, depth, 128), BF16),
            pltpu.VMEM((CH * across, SEQS), F32),
            pltpu.VMEM((GROUP, pairs, CH * CH), F32),
            pltpu.VMEM((CH * CH, pairs), F32),
            pltpu.VMEM((8, pairs), F32),
            pltpu.SemaphoreType.DMA((2, CH // GROUP)),
        ],
        compiler_params=pltpu.CompilerParams(vmem_limit_bytes=60 * 1024 * 1024),
        cost_estimate=pl.CostEstimate(
            flops=10 * count * across * CH * CH * SEQS * 2,
            bytes_accessed=32 * 1024 * 1024,
            transcendentals=0,
        ),
    )(lanes, rows, weights, bias, upstream)


def exchange(x, axis, groups=None):
    return lax.all_to_all(
        x, axis, split_axis=0, concat_axis=0, axis_index_groups=groups, tiled=True
    )


def everywhere(x, axis, groups=None):
    members = lax.axis_size(axis) if groups is None else len(groups[0])
    copies = jnp.broadcast_to(x[None], (members,) + x.shape)
    return exchange(copies, axis, groups)


def two_parts(x):
    high = x.astype(BF16)
    low = (x - high.astype(F32)).astype(BF16)
    return jnp.concatenate([high, low, jnp.zeros((TILE - 2, x.shape[1]), BF16)], axis=0)


def one_part(x):
    return jnp.sum(x[:2], axis=0, keepdims=True)


def local(left_features, right_features, weight, bias, upstream):
    rows_n, cols_n = lax.axis_size("row"), lax.axis_size("col")
    own, pairs = left_features.shape[0], weight.shape[1]
    count, across = upstream.shape[0], upstream.shape[1]
    to_part = [(o, (o % rows_n) * cols_n + o // rows_n) for o in range(rows_n * cols_n)]
    to_owner = [(b, a) for a, b in to_part]
    both = ("row", "col")
    same_core = [list(range(k, cols_n, 2)) for k in range(2)]
    other_core = [(k, k ^ 1) for k in range(cols_n)]
    n_own = 2 * own * CH

    mine = jnp.concatenate([left_features, right_features], axis=0)
    mine = mine.reshape(2 * own, SEQS, CH).transpose(0, 2, 1).reshape(2, own * CH, SEQS)
    turned = weight.reshape(CH, CH, pairs).transpose(1, 0, 2).reshape(CH * CH, pairs)
    weights = jnp.stack([turned, weight])
    part = lax.ppermute(mine, both, to_part)
    half = everywhere(mine, "col", same_core)
    other = lax.ppermute(half, "col", other_core)
    rows = everywhere(part, "row")
    second = (lax.axis_index("col") & 1) == 1
    lanes = jnp.stack([jnp.where(second, other, half), jnp.where(second, half, other)], axis=1)
    lanes = lanes.transpose(2, 0, 1, 3, 4).reshape(2, count * CH, SEQS)
    rows = rows.reshape(rows_n, 2, own, CH // GROUP, GROUP, SEQS)
    rows = rows.transpose(1, 4, 3, 0, 2, 5).reshape(2, CH * across, SEQS)
    pair_out, g_terms, to_rows = pair_block(
        lanes, rows, weights, bias.reshape(1, pairs), upstream, rows_n
    )
    n_slice = CH * CH // rows_n

    def with_bias(x):
        return jnp.concatenate(
            [x[:n_slice].astype(BF16), two_parts(one_part(x[n_slice:]))], axis=0
        )

    sent = exchange(to_rows, "row")
    core = (lax.axis_index("col") & 1).astype(jnp.int32).reshape(1)
    to_cols, theirs = lane_block(core, g_terms, rows, own, n_own)
    other = lax.ppermute(theirs, "col", other_core)
    summed = jnp.sum(sent.astype(F32), axis=0)
    part_grads = lax.ppermute(summed[:n_own].astype(BF16), both, to_owner)
    shared = with_bias(summed[n_own:])
    shared_other = lax.ppermute(shared, "col", other_core)
    shared = with_bias(shared.astype(F32) + shared_other.astype(F32))
    mine = (to_cols[:, :n_own].astype(F32) + other.astype(F32)).astype(BF16)
    shared = jnp.broadcast_to(shared[None], (cols_n // 2,) + shared.shape)
    sent = exchange(jnp.concatenate([mine, shared], axis=1), "col", same_core)
    summed = jnp.sum(sent.astype(F32), axis=0)
    grad_weight = everywhere(summed[n_own : n_own + n_slice].astype(BF16), "row")
    grad_weight = grad_weight.astype(F32).reshape(CH * CH, pairs)
    grad_bias = one_part(summed[n_own + n_slice :]).reshape(pairs)
    grads = summed[:n_own] + part_grads.astype(F32)
    grads = grads.reshape(2, own, CH, SEQS).transpose(0, 1, 3, 2).reshape(2, own, SEQS * CH)
    grads = grads.astype(BF16)
    return pair_out, grads[0], grads[1], grad_weight, grad_bias


def solution(mesh):
    placed = (P(("row", "col"), None), P(("row", "col"), None), P(), P(), P("row", "col", None))
    return jax.shard_map(
        local,
        mesh=mesh,
        in_specs=placed,
        out_specs=(
            P("row", "col", None),
            P(("row", "col"), None),
            P(("row", "col"), None),
            P(),
            P(),
        ),
        check_vma=False,
    )
```

```python
import functools

import jax
import jax.numpy as jnp
from jax import lax
from jax.experimental import pallas as pl
from jax.experimental.pallas import tpu as pltpu
from jax.sharding import PartitionSpec as P


CH = 32
SEQS = 128
GROUP = 4
BLOCK = 48
TILE = 16
BF16 = jnp.bfloat16
F32 = jnp.float32


def contract(a, b, dims):
    numbers = (((dims[0],), (dims[1],)), ((), ()))
    return lax.dot_general(a, b, numbers, preferred_element_type=F32)


def spread(parts, odd, high):
    once = [jnp.where(odd, parts[(r + 1) % GROUP], parts[r]) for r in range(GROUP)]
    twice = [jnp.where(high, once[(r + 2) % GROUP], once[r]) for r in range(GROUP)]
    return [twice[-q % GROUP] for q in range(GROUP)]


def unturned(wide, turn):
    if turn == 0:
        return wide
    return jnp.concatenate(
        [
            pltpu.roll(wide[:, n * 128 : (n + 1) * 128], 128 - CH * turn, 1)
            for n in range(wide.shape[1] // 128)
        ],
        axis=1,
    )


def to_tiles(ref, at, wide):
    for n in range(wide.shape[1] // 128):
        ref[at, n] = wide[:, n * 128 : (n + 1) * 128]


def from_tiles(ref, at, first=0, count=None):
    count = ref.shape[1] if count is None else count
    return jnp.concatenate([ref[at, first + n] for n in range(count)], axis=1)


def pair_kernel(
    across,
    lane_ref,
    row_ref,
    weight_ref,
    bias_ref,
    up_ref,
    pair_ref,
    grads_ref,
    send_ref,
    squares,
    products,
    packed,
    g_packed,
    g_tiles,
    drow_acc,
    dweight_acc,
    dweight_sum,
    dbias_acc,
    sent_sems,
):
    term = pl.program_id(0)
    quarters = CH // GROUP
    groups = lane_ref.shape[1] // (CH * GROUP)
    depth = quarters * across
    scale = 1.0 / SEQS
    lane = lax.broadcasted_iota(jnp.int32, (TILE, 128), 1) // CH
    odd = (lane % 2).astype(F32).astype(BF16) > 0.5
    high = (lane // 2).astype(F32).astype(BF16) > 0.5

    def turned_lanes(m):
        return jnp.concatenate(
            [
                lane_ref[0, pl.ds((GROUP * g + (p - m) % GROUP) * CH, CH), :]
                for g in range(groups)
                for p in range(GROUP)
            ],
            axis=0,
        )

    def turned_weight(q):
        return jnp.concatenate(
            [
                weight_ref[0, pl.ds((GROUP * k + (p - q) % GROUP) * CH, CH), :]
                for k in range(quarters)
                for p in range(GROUP)
            ],
            axis=0,
        )

    for m in range(GROUP):
        outer = contract(row_ref[0, m * depth : (m + 1) * depth, :], turned_lanes(m), (1, 1))
        to_tiles(products, m, (outer * scale).astype(BF16))

    def by_pair(k, _):
        from_rows = k * across
        for g in range(groups):
            for t in range(0, across, TILE):
                parts = [
                    products[m, g, pl.ds(from_rows + t, TILE), :] for m in range(GROUP)
                ]
                for q, tile in enumerate(spread(parts, odd, high)):
                    packed[q, k, pl.ds(g * across + t, TILE), :] = tile
        return _

    for k in range(quarters):
        by_pair(k, 0)
    for q in range(GROUP):
        outer = from_tiles(packed, q)
        weight_q = turned_weight(q)
        pre = jnp.dot(outer, weight_q, preferred_element_type=F32) + bias_ref[...]
        active = jnp.maximum(pre, 0.0)
        squared = active * active
        up = jnp.concatenate([up_ref[GROUP * g + q] for g in range(groups)], axis=0)
        d_pre = (active * up.astype(F32)).astype(BF16)

        for g in range(groups):
            place = GROUP * g + q
            here = squared[g * across : (g + 1) * across]
            pair_ref[GROUP * g + q] = ((here + squares[place]) * 0.5).astype(BF16)
            squares[place] = here
        to_tiles(g_packed, q, contract(d_pre, weight_q, (1, 1)).astype(BF16))
        dweight_acc[q] = contract(d_pre, outer, (0, 0))
        d_bias = jnp.sum(d_pre.astype(F32).reshape(groups * across // 8, 8, 128), axis=0)
        dbias_acc[...] = d_bias + jnp.where((term == 0) & (q == 0), 0.0, dbias_acc[...])

    def g_copy(term, k):
        rows = pl.ds(pl.multiple_of(k * across, TILE), across)
        return pltpu.make_async_copy(
            g_tiles.at[term, :, :, rows, :], grads_ref.at[term, :, :, rows, :], sent_sems.at[term, k]
        )

    def by_channel(k, _):
        to_rows = pl.multiple_of(k * across, TILE)
        for g in range(groups):
            for t in range(0, across, TILE):
                parts = [
                    g_packed[q, k, pl.ds(g * across + t, TILE), :] for q in range(GROUP)
                ]
                for m, tile in enumerate(spread(parts, odd, high)):
                    g_tiles[term, m, g, pl.ds(to_rows + t, TILE), :] = tile
        g_copy(term, k).start()
        return _

    lax.fori_loop(0, quarters, by_channel, 0)

    for m in range(GROUP):
        tiles = from_tiles(g_tiles.at[term], m)
        drow_acc[pl.ds(m * depth, depth)] = jnp.dot(
            tiles, turned_lanes(m), preferred_element_type=F32
        )

    by_channel_rows = jnp.stack(
        [
            drow_acc[pl.ds(m * depth + k * across, across), :]
            for k in range(quarters)
            for m in range(GROUP)
        ]
    )
    sent = (jnp.swapaxes(by_channel_rows, 0, 1) * scale).astype(BF16)
    sent = sent.reshape(send_ref.shape[0], -1, SEQS)
    count = sent.shape[1]
    total = dweight_acc[0]
    for q in range(1, GROUP):
        total = total + unturned(dweight_acc[q], q)
    flat = total.T

    @pl.when(term == 0)
    def _():
        send_ref[:, count : 2 * count, :] = sent
        dweight_sum[...] = jnp.swapaxes(flat.reshape(CH, CH, -1), 0, 1).reshape(flat.shape)

    @pl.when(term == 1)
    def _():
        send_ref[:, :count, :] = sent
        whole = (dweight_sum[...] + flat).astype(BF16)
        peers = send_ref.shape[0]
        end = 2 * count + whole.shape[0] // peers
        send_ref[:, 2 * count : end, :] = whole.reshape(peers, -1, whole.shape[1])
        d_bias = jnp.sum(dbias_acc[...], axis=0, keepdims=True)
        first = d_bias.astype(BF16).astype(F32)
        place = lax.broadcasted_iota(jnp.int32, (TILE, 128), 0)
        rows = jnp.where(place == 0, first, jnp.where(place == 1, d_bias - first, 0.0))
        for r in range(peers):
            send_ref[r, end : end + TILE, :] = rows.astype(BF16)

    @pl.when(term == 1)
    def _():
        for t in range(2):
            for k in range(quarters):
                g_copy(t, k).wait()


def lane_kernel(across, core_ref, grads_ref, row_ref, mine_ref, theirs_ref, cols_ref, row_t):
    term, step = pl.program_id(0), pl.program_id(1)
    depth = CH // GROUP * across
    _, owners, height, _ = cols_ref.shape
    own = height // (2 * CH)
    core = core_ref[0]

    @pl.when(step == 0)
    def _():
        for m in range(GROUP):
            row_t[m] = row_ref[0, m * depth : (m + 1) * depth, :].T

    for n in range(0, BLOCK * CH, 256):
        d_lane = None
        for m in range(GROUP):
            wide = jnp.dot(
                row_t[m],
                from_tiles(grads_ref.at[0], m, n // 128, 2),
                preferred_element_type=F32,
            )
            wide = unturned(wide, m)
            d_lane = wide if d_lane is None else d_lane + wide
        d_lane = (d_lane.T * (1.0 / SEQS)).astype(BF16)
        for r in range(256 // CH):
            residue = step * BLOCK + n // CH + r
            owner = residue // own
            place = (owner + core) % 2
            to_row = pl.multiple_of((term * own + residue % own) * CH, CH)
            cols_ref[place, owner // 2, pl.ds(to_row, CH), :] = d_lane[r * CH : (r + 1) * CH]

    @pl.when((term == 1) & (step == pl.num_programs(1) - 1))
    def _():
        mine_ref[:, : 2 * own * CH, :] = cols_ref[0]
        theirs_ref[...] = cols_ref[1]


def lane_block(core, grads, rows, own, height):
    _, _, groups, depth, _ = grads.shape
    across = depth // (CH // GROUP)
    steps = groups * GROUP // BLOCK
    owners = steps * BLOCK // own
    return pl.pallas_call(
        functools.partial(lane_kernel, across),
        grid=(2, steps),
        in_specs=[
            pl.BlockSpec(memory_space=pltpu.SMEM),
            pl.BlockSpec(
                (1, GROUP, BLOCK // GROUP, depth, 128), lambda t, s: (t, 0, s, 0, 0)
            ),
            pl.BlockSpec((1, CH * across, SEQS), lambda t, s: (1 - t, 0, 0)),
        ],
        out_specs=[
            pl.BlockSpec((owners // 2, height, SEQS), lambda t, s: (0, 0, 0)),
            pl.BlockSpec((owners // 2, 2 * own * CH, SEQS), lambda t, s: (0, 0, 0)),
        ],
        out_shape=[
            jax.ShapeDtypeStruct((owners // 2, height, SEQS), BF16),
            jax.ShapeDtypeStruct((owners // 2, 2 * own * CH, SEQS), BF16),
        ],
        scratch_shapes=[
            pltpu.VMEM((2, owners // 2, 2 * own * CH, SEQS), BF16),
            pltpu.VMEM((GROUP, SEQS, depth), BF16),
        ],
        compiler_params=pltpu.CompilerParams(vmem_limit_bytes=40 * 1024 * 1024),
        cost_estimate=pl.CostEstimate(
            flops=4 * steps * BLOCK * across * CH * CH * SEQS,
            bytes_accessed=24 * 1024 * 1024,
            transcendentals=0,
        ),
    )(core, grads, rows)


def pair_block(lanes, rows, weights, bias, upstream, row_peers):
    count, across, pairs = upstream.shape
    width = count * CH
    depth = CH // GROUP * across
    high = count // GROUP * across
    sent = 2 * CH * across // row_peers + CH * CH // row_peers + TILE
    return pl.pallas_call(
        functools.partial(pair_kernel, across),
        grid=(2,),
        in_specs=[
            pl.BlockSpec((1, width, SEQS), lambda t: (t, 0, 0)),
            pl.BlockSpec((1, CH * across, SEQS), lambda t: (1 - t, 0, 0)),
            pl.BlockSpec((1, CH * CH, pairs), lambda t: (t, 0, 0)),
            pl.BlockSpec((1, pairs), lambda t: (0, 0)),
            pl.BlockSpec((count, across, pairs), lambda t: (0, 0, 0)),
        ],
        out_specs=[
            pl.BlockSpec((count, across, pairs), lambda t: (0, 0, 0)),
            pl.BlockSpec(memory_space=pl.ANY),
            pl.BlockSpec((row_peers, sent, SEQS), lambda t: (0, 0, 0)),
        ],
        out_shape=[
            jax.ShapeDtypeStruct((count, across, pairs), BF16),
            jax.ShapeDtypeStruct((2, GROUP, width // 128, depth, 128), BF16),
            jax.ShapeDtypeStruct((row_peers, sent, SEQS), BF16),
        ],
        scratch_shapes=[
            pltpu.VMEM((count, across, pairs), F32),
            pltpu.VMEM((GROUP, width // 128, depth, 128), BF16),
            pltpu.VMEM((GROUP, CH // GROUP, high, 128), BF16),
            pltpu.VMEM((GROUP, CH // GROUP, high, 128), BF16),
            pltpu.VMEM((2, GROUP, width // 128, depth, 128), BF16),
            pltpu.VMEM((CH * across, SEQS), F32),
            pltpu.VMEM((GROUP, pairs, CH * CH), F32),
            pltpu.VMEM((CH * CH, pairs), F32),
            pltpu.VMEM((8, pairs), F32),
            pltpu.SemaphoreType.DMA((2, CH // GROUP)),
        ],
        compiler_params=pltpu.CompilerParams(vmem_limit_bytes=60 * 1024 * 1024),
        cost_estimate=pl.CostEstimate(
            flops=10 * count * across * CH * CH * SEQS * 2,
            bytes_accessed=32 * 1024 * 1024,
            transcendentals=0,
        ),
    )(lanes, rows, weights, bias, upstream)


def exchange(x, axis, groups=None):
    return lax.all_to_all(
        x, axis, split_axis=0, concat_axis=0, axis_index_groups=groups, tiled=True
    )


def everywhere(x, axis, groups=None):
    members = lax.axis_size(axis) if groups is None else len(groups[0])
    copies = jnp.broadcast_to(x[None], (members,) + x.shape)
    return exchange(copies, axis, groups)


def two_parts(x):
    high = x.astype(BF16)
    low = (x - high.astype(F32)).astype(BF16)
    return jnp.concatenate([high, low, jnp.zeros((TILE - 2, x.shape[1]), BF16)], axis=0)


def one_part(x):
    return jnp.sum(x[:2], axis=0, keepdims=True)


def local(left_features, right_features, weight, bias, upstream):
    rows_n, cols_n = lax.axis_size("row"), lax.axis_size("col")
    own, pairs = left_features.shape[0], weight.shape[1]
    count, across = upstream.shape[0], upstream.shape[1]
    to_part = [(o, (o % rows_n) * cols_n + o // rows_n) for o in range(rows_n * cols_n)]
    to_owner = [(b, a) for a, b in to_part]
    both = ("row", "col")
    same_core = [list(range(k, cols_n, 2)) for k in range(2)]
    other_core = [(k, k ^ 1) for k in range(cols_n)]
    n_own = 2 * own * CH

    mine = jnp.concatenate([left_features, right_features], axis=0)
    mine = mine.reshape(2 * own, SEQS, CH).transpose(0, 2, 1).reshape(2, own * CH, SEQS)
    turned = weight.reshape(CH, CH, pairs).transpose(1, 0, 2).reshape(CH * CH, pairs)
    weights = jnp.stack([turned, weight])
    part = lax.ppermute(mine, both, to_part)
    half = everywhere(mine, "col", same_core)
    other = lax.ppermute(half, "col", other_core)
    rows = everywhere(part, "row")
    second = (lax.axis_index("col") & 1) == 1
    lanes = jnp.stack([jnp.where(second, other, half), jnp.where(second, half, other)], axis=1)
    lanes = lanes.transpose(2, 0, 1, 3, 4).reshape(2, count * CH, SEQS)
    rows = rows.reshape(rows_n, 2, own, CH // GROUP, GROUP, SEQS)
    rows = rows.transpose(1, 4, 3, 0, 2, 5).reshape(2, CH * across, SEQS)
    pair_out, g_terms, to_rows = pair_block(
        lanes, rows, weights, bias.reshape(1, pairs), upstream, rows_n
    )
    n_slice = CH * CH // rows_n

    def with_bias(x):
        return jnp.concatenate(
            [x[:n_slice].astype(BF16), two_parts(one_part(x[n_slice:]))], axis=0
        )

    sent = exchange(to_rows, "row")
    core = (lax.axis_index("col") & 1).astype(jnp.int32).reshape(1)
    to_cols, theirs = lane_block(core, g_terms, rows, own, n_own)
    other = lax.ppermute(theirs, "col", other_core)
    summed = jnp.sum(sent.astype(F32), axis=0)
    part_grads = lax.ppermute(summed[:n_own].astype(BF16), both, to_owner)
    shared = with_bias(summed[n_own:])
    shared_other = lax.ppermute(shared, "col", other_core)
    shared = with_bias(shared.astype(F32) + shared_other.astype(F32))
    mine = (to_cols[:, :n_own].astype(F32) + other.astype(F32)).astype(BF16)
    shared = jnp.broadcast_to(shared[None], (cols_n // 2,) + shared.shape)
    sent = exchange(jnp.concatenate([mine, shared], axis=1), "col", same_core)
    summed = jnp.sum(sent.astype(F32), axis=0)
    grad_weight = everywhere(summed[n_own : n_own + n_slice].astype(BF16), "row")
    grad_weight = grad_weight.astype(F32).reshape(CH * CH, pairs)
    grad_bias = one_part(summed[n_own + n_slice :]).reshape(pairs)
    grads = summed[:n_own] + part_grads.astype(F32)
    grads = grads.reshape(2, own, CH, SEQS).transpose(0, 1, 3, 2).reshape(2, own, SEQS * CH)
    grads = grads.astype(BF16)
    return pair_out, grads[0], grads[1], grad_weight, grad_bias


def solution(mesh):
    placed = (P(("row", "col"), None), P(("row", "col"), None), P(), P(), P("row", "col", None))
    return jax.shard_map(
        local,
        mesh=mesh,
        in_specs=placed,
        out_specs=(
            P("row", "col", None),
            P(("row", "col"), None),
            P(("row", "col"), None),
            P(),
            P(),
        ),
        check_vma=False,
    )
```
